16 devices in a mesh: ez: 2 (over z), ey: 2 (over y), ex: 4 (over x, core).
Axes of the slice: x: 2, y: 2, z: 2, core: 2. Of those that a mesh axis runs over, the one named last changes fastest.
Arguments:
- x_tokens: bfloat16 [8192, 1024], P(('ez', 'ey', 'ex'))
- expert_ids: int32 [8192, 8], P(('ez', 'ey', 'ex'))
- gate_vals: float32 [8192, 8], P(('ez', 'ey', 'ex'))
- w_gate: bfloat16 [32, 1024, 512], P(('ex', 'ey', 'ez'))
- w_up: bfloat16 [32, 1024, 512], P(('ex', 'ey', 'ez'))
- w_down: bfloat16 [32, 512, 1024], P(('ex', 'ey', 'ez'))
Outputs:
- output: bfloat16 [8192, 1024], P(('ez', 'ey', 'ex'))
All inputs are finite; a program needn't handle non-finite values.
Results may differ from the reference program's by a relative error of at most 0.001.
Values are sent between devices in bfloat16 or wider.
A program may use at most 1 GiB of HBM per device.

```python
import jax
import jax.numpy as jnp
from jax import lax

HIDDEN = 1024
FFN_DIM = 512
EXPERTS = 32
TOP_K = 8
TOK_DEV = 512
DEVICES = 16
GROUPS = 8

TOKENS_ALL = DEVICES * TOK_DEV
CAP_EXPERT = 2 * DEVICES * TOK_DEV * TOP_K // EXPERTS


def draw_routing(route_key):
    perm_key, group_key = jax.random.split(route_key)
    group_size = EXPERTS // GROUPS
    pair_count = group_size // 2
    pick_groups = TOP_K // 2
    perm_score = jax.random.randint(perm_key, (DEVICES, GROUPS, group_size), 0, 1 << 20)
    inner_perm = jnp.argsort(perm_score * group_size + jnp.arange(group_size), axis=-1)
    inner_perm = inner_perm.at[:, :, 2].set(inner_perm[:, :, 0])
    group_score = jax.random.randint(group_key, (DEVICES, GROUPS), 0, 1 << 20)
    group_perm = jnp.argsort(group_score * GROUPS + jnp.arange(GROUPS), axis=-1)
    visit_idx = jnp.arange(TOK_DEV)[:, None] * pick_groups + jnp.arange(pick_groups)[None, :]
    dev_idx = jnp.arange(DEVICES)[:, None, None]
    group_id = group_perm[dev_idx, visit_idx[None] % GROUPS]
    pair_pos = 2 * ((visit_idx // GROUPS) % pair_count)[None]
    first_pick = inner_perm[dev_idx, group_id, pair_pos]
    second_pick = inner_perm[dev_idx, group_id, pair_pos + 1]
    local_pick = jnp.stack([first_pick, second_pick], axis=-1)
    expert_ids = group_id[:, :, :, None] * group_size + local_pick
    return expert_ids.reshape(TOKENS_ALL, TOP_K).astype(jnp.int32)


def setup_inputs(seed: int = 0) -> dict:
    base_key = jax.random.key(seed)
    key_x, key_gate, key_one, key_three, key_two, key_route = jax.random.split(base_key, 6)
    x_tokens = jax.random.normal(key_x, (TOKENS_ALL, HIDDEN), jnp.float32)
    gate_raw = jax.random.uniform(key_gate, (TOKENS_ALL, TOP_K), jnp.float32, 0.5, 1.5)
    gate_vals = 2.5 * gate_raw / jnp.sum(gate_raw, axis=1, keepdims=True)
    w_gate = jax.random.normal(key_one, (EXPERTS, HIDDEN, FFN_DIM), jnp.float32) * HIDDEN ** -0.5
    w_up = jax.random.normal(key_three, (EXPERTS, HIDDEN, FFN_DIM), jnp.float32) * HIDDEN ** -0.5
    w_down = jax.random.normal(key_two, (EXPERTS, FFN_DIM, HIDDEN), jnp.float32) * FFN_DIM ** -0.5
    return {
        'x_tokens': x_tokens.astype(jnp.bfloat16),
        'expert_ids': draw_routing(key_route),
        'gate_vals': gate_vals,
        'w_gate': w_gate.astype(jnp.bfloat16),
        'w_up': w_up.astype(jnp.bfloat16),
        'w_down': w_down.astype(jnp.bfloat16),
    }


def reference(x_tokens, expert_ids, gate_vals, w_gate, w_up, w_down):
    flat_ids = expert_ids.reshape(-1)
    flat_gates = gate_vals.reshape(-1)
    pair_tok = jnp.arange(TOKENS_ALL * TOP_K) // TOP_K
    slot_pos = jnp.arange(CAP_EXPERT)

    def expert_step(acc_sum, scan_in):
        expert, w_one, w_three, w_two = scan_in
        chosen = flat_ids == expert
        n_chosen = jnp.sum(chosen.astype(jnp.int32))
        pair_sel = jnp.nonzero(chosen, size=CAP_EXPERT, fill_value=0)[0]
        tok_sel = pair_tok[pair_sel]
        weight = jnp.where(slot_pos < n_chosen, flat_gates[pair_sel], 0.0)
        tok_rows = x_tokens[tok_sel]
        h_gate = jnp.dot(tok_rows, w_one, preferred_element_type=jnp.float32)
        h_up = jnp.dot(tok_rows, w_three, preferred_element_type=jnp.float32)
        act_bf = (jax.nn.silu(h_gate) * h_up).astype(jnp.bfloat16)
        exp_out = jnp.dot(act_bf, w_two, preferred_element_type=jnp.float32).astype(jnp.bfloat16)
        acc_sum = acc_sum.at[tok_sel].add(weight[:, None] * exp_out.astype(jnp.float32))
        return acc_sum, None

    acc_init = jnp.zeros((TOKENS_ALL, HIDDEN), jnp.float32)
    moe_sum = lax.scan(expert_step, acc_init, (jnp.arange(EXPERTS), w_gate, w_up, w_down))[0]
    return (x_tokens.astype(jnp.float32) + moe_sum).astype(jnp.bfloat16)
```

```python
import jax
import jax.numpy as jnp
from jax import lax
from jax.experimental import pallas as pl
from jax.experimental.pallas import tpu as pltpu
from jax.sharding import PartitionSpec as P

TOKEN_AXES = ('ez', 'ey', 'ex')
EXPERT_AXES = ('ex', 'ey', 'ez')
MESH = pl.DeviceIdType.MESH

CHIP_MASKS = (0, 2, 4, 8, 6, 10, 12, 14)
Q_OF = {m: q for q, m in enumerate(CHIP_MASKS)}
ORDERS = ((2, 4, 8), (4, 8, 2), (8, 2, 4))
AG_PARTS = ((0, 176), (176, 176), (352, 160))
RS_PARTS = ((0, 176), (176, 168), (344, 168))
HALF = 256


def slot_of(mask):
    return 2 * Q_OF[mask & 14] + (mask & 1)


def peer(mask):
    z, y, e = lax.axis_index('ez'), lax.axis_index('ey'), lax.axis_index('ex')
    x, c = e // 2, e % 2
    z = 1 - z if mask & 8 else z
    y = 1 - y if mask & 4 else y
    x = 1 - x if mask & 2 else x
    c = 1 - c if mask & 1 else c
    return z, y, 2 * x + c


def moe_kernel(x_hbm, g_hbm, w1_hbm, w3_hbm, w2_hbm, y_hbm,
               w1, w3, w2, x_all, g_all, act, acc, rs, dd_in,
               load_sem, g_send, g_recv, ag_send, ag_recv, xd_send, xd_recv,
               rs_send, rs_recv, dd_send, dd_recv, dd_free):
    tok, hid = x_hbm.shape
    partner = peer(1)

    def remote(src, dst, ssem, rsem, mask):
        return pltpu.make_async_remote_copy(src, dst, ssem, rsem, device_id=peer(mask), device_id_type=MESH)

    def expert_place(mask):
        z, y, e = peer(mask)
        return e * 4 + y * 2 + z

    def gate_copy(mask):
        return remote(g_hbm.at[expert_place(mask)], g_all.at[slot_of(mask)], g_send.at[mask], g_recv.at[mask], mask)

    def ag_sources(p):
        d0, d1, d2 = ORDERS[p]
        return ((0, d0), (0, d1), (0, d2), (d0, d1), (d0, d2), (d1, d2), (d0 ^ d1, d2))

    def ag_copy(p, k):
        mask, axis = ag_sources(p)[k]
        r0, n = AG_PARTS[p]
        return remote(x_all.at[slot_of(mask), pl.ds(r0, n)], x_all.at[slot_of(mask ^ axis), pl.ds(r0, n)],
                      ag_send.at[p, k], ag_recv.at[p, k], axis)

    def x_partner_copy(q, p):
        r0, n = (0, tok) if q == 0 else AG_PARTS[p]
        return remote(x_all.at[2 * q, pl.ds(r0, n)], x_all.at[2 * q + 1, pl.ds(r0, n)], xd_send.at[q, p], xd_recv.at[q, p], 1)

    def rs_moves(p):
        e0, e1, e2 = ORDERS[p]
        first = {0: (6, 10), 1: (6, 12), 2: (10, 12)}[p]
        return ((e0, e0), (first[0], e0), (14, e0), (first[1], e0), (e1 ^ e2, e1), (e1, e1), (e2, e2))

    def rs_copy(p, k):
        mask, axis = rs_moves(p)[k]
        r0, n = RS_PARTS[p]
        return remote(acc.at[Q_OF[mask], pl.ds(r0, n)], rs.at[k, pl.ds(r0, n)], rs_send.at[p, k], rs_recv.at[p, k], axis)

    def rs_add(p, k):
        mask, axis = rs_moves(p)[k]
        q = Q_OF[mask ^ axis]
        r0, n = RS_PARTS[p]
        rs_copy(p, k).wait_recv()

        @pl.loop(0, n // 8)
        def _(i):
            rows = pl.ds(pl.multiple_of(r0 + i * 8, 8), 8)
            acc[q, rows, :] = acc[q, rows, :] + rs[k, rows, :]

    def partial_copy(h):
        rows = pl.ds(pl.multiple_of(h * HALF, HALF), HALF)
        return remote(acc.at[8, rows], dd_in.at[h], dd_send.at[h], dd_recv.at[h], 1)

    loads = [pltpu.make_async_copy(s, d, load_sem.at[i]) for i, (s, d) in enumerate((
        (x_hbm, x_all.at[0]), (g_hbm.at[expert_place(0)], g_all.at[0]), (w1_hbm, w1), (w3_hbm, w3), (w2_hbm, w2)))]

    for c in loads:
        c.start()
    barrier = pltpu.get_barrier_semaphore()
    for mask in range(1, 16):
        pl.semaphore_signal(barrier, inc=1, device_id=peer(mask), device_id_type=MESH)
    pl.semaphore_wait(barrier, 15)
    for mask in range(1, 16):
        gate_copy(mask).start()
    loads[0].wait()
    for k in range(3):
        for p in range(3):
            ag_copy(p, k).start()
    x_partner_copy(0, 0).start()
    for c in loads[1:]:
        c.wait()
    for mask in range(1, 16):
        gate_copy(mask).wait_recv()

    def arrived(k, onward):
        for p in range(3):
            ag_copy(p, k).wait_recv()
            for j in onward:
                ag_copy(p, j).start()
            mask, axis = ag_sources(p)[k]
            x_partner_copy(Q_OF[mask ^ axis], p).start()

    def x_ready(q):
        if q == 0:
            x_partner_copy(0, 0).wait_recv()
        else:
            for p in range(3):
                x_partner_copy(q, p).wait_recv()

    def events(q):
        if q == 1:
            arrived(0, (3, 4))
            arrived(1, (5,))
            arrived(2, ())
        if q == 2:
            arrived(3, (6,))
            rs_copy(0, 0).start()
        if q == 3:
            arrived(4, ())
            rs_copy(1, 0).start()
        if q == 4:
            arrived(5, ())
            rs_copy(2, 0).start()
        if q == 5:
            arrived(6, ())
            rs_copy(0, 1).start()
            rs_copy(1, 1).start()
        if q == 6:
            rs_copy(2, 1).start()
        x_ready(q)

    @pl.loop(0, 32)
    def _(step):
        q, turn = step // 4, step % 4
        other = 1 - turn // 2
        h = turn % 2
        for i in range(8):
            @pl.when(step == 4 * i)
            def _(i=i):
                events(i)

        slot = 2 * q + other
        into = q + other * (8 - q)
        r0 = pl.multiple_of(h * HALF, HALF)

        @pl.when(jnp.logical_and(other == 1, q > 0))
        def _():
            partial_copy(h).wait_send()

        gate = g_all[slot].T
        cols = []
        for l in range(2):
            halves = [jnp.where(h == 0, gate[:, 2 * i + l:2 * i + l + 1], gate[:, 4 + 2 * i + l:5 + 2 * i + l]) for i in range(2)]
            cols.append(jnp.concatenate(halves, axis=0))
        for l in range(2):
            for n in range(2):
                cs = slice(n * 256, n * 256 + 256)
                x_in = x_all[slot, pl.ds(r0, HALF), :]
                h1 = jnp.dot(x_in, w1[l, :, cs], preferred_element_type=jnp.float32)
                h3 = jnp.dot(x_in, w3[l, :, cs], preferred_element_type=jnp.float32)
                act[l, :, cs] = (h1 * jax.nn.sigmoid(h1) * h3).astype(jnp.bfloat16)
        for n in range(4):
            cs = slice(n * 256, n * 256 + 256)
            total = None
            for l in range(2):
                o = jnp.dot(act[l], w2[l, :, cs], preferred_element_type=jnp.float32)
                o = o.astype(jnp.bfloat16).astype(jnp.float32)
                term = jnp.where(cols[l] > 0, cols[l] * o, 0.0)
                total = term if total is None else total + term
            acc[into, pl.ds(r0, HALF), cs] = total

        @pl.when(other == 1)
        def _():
            @pl.when(q > 0)
            def _():
                pl.semaphore_wait(dd_free.at[h], 1)
            partial_copy(h).start()

        @pl.when(other == 0)
        def _():
            partial_copy(h).wait_recv()

            @pl.loop(0, HALF // 8)
            def _(i):
                rows = pl.ds(pl.multiple_of(i * 8, 8), 8)
                out = pl.ds(pl.multiple_of(r0 + i * 8, 8), 8)
                acc[q, out, :] = acc[q, out, :] + dd_in[h, rows, :]

            @pl.when(q < 7)
            def _():
                pl.semaphore_signal(dd_free.at[h], inc=1, device_id=partner, device_id_type=MESH)

    for p in range(3):
        rs_copy(p, 2).start()
    for p in range(3):
        rs_copy(p, 3).start()
    for k in (0, 1):
        for p in range(3):
            rs_add(p, k)
    for p in range(3):
        rs_add(p, 2)
        rs_copy(p, 4).start()
    for p in range(3):
        rs_add(p, 3)
        rs_copy(p, 5).start()
    for p in range(3):
        rs_add(p, 4)
        rs_copy(p, 6).start()
    for p in range(3):
        rs_add(p, 5)
    for p in range(3):
        rs_copy(p, 6).wait_recv()

    @pl.loop(0, tok // 16)
    def _(i):
        rows = pl.ds(pl.multiple_of(i * 16, 16), 16)
        x_all[1, rows, :] = (x_all[0, rows, :].astype(jnp.float32) + (acc[0, rows, :] + rs[6, rows, :])).astype(jnp.bfloat16)

    store = pltpu.make_async_copy(x_all.at[1], y_hbm, load_sem.at[0])
    store.start()
    for mask in range(1, 16):
        gate_copy(mask).wait_send()
    for p in range(3):
        for k in range(7):
            ag_copy(p, k).wait_send()
            rs_copy(p, k).wait_send()
    x_partner_copy(0, 0).wait_send()
    for q in range(1, 8):
        for p in range(3):
            x_partner_copy(q, p).wait_send()
    for h in range(2):
        partial_copy(h).wait_send()
    store.wait()


def solution(mesh):
    n_dev = mesh.shape['ez'] * mesh.shape['ey'] * mesh.shape['ex']

    def local_layer(x_loc, ids_loc, gates_loc, w_g, w_u, w_d):
        tok, hid = x_loc.shape
        n_local, _, ffn = w_g.shape
        n_exp = n_local * n_dev
        hit = ids_loc[:, :, None] == jnp.arange(n_exp)[None, None, :]
        dense_g = jnp.sum(jnp.where(hit, gates_loc[:, :, None], 0.0), axis=1)
        tiles = dense_g.T.reshape(n_dev, n_local, 4, 128).transpose(0, 2, 1, 3).reshape(n_dev, 8, 128)
        hbm = pl.BlockSpec(memory_space=pl.ANY)
        dma = pltpu.SemaphoreType.DMA
        return pl.pallas_call(
            moe_kernel,
            out_shape=jax.ShapeDtypeStruct((tok, hid), jnp.bfloat16),
            in_specs=[hbm] * 5,
            out_specs=hbm,
            scratch_shapes=[
                pltpu.VMEM((n_local, hid, ffn), jnp.bfloat16),
                pltpu.VMEM((n_local, hid, ffn), jnp.bfloat16),
                pltpu.VMEM((n_local, ffn, hid), jnp.bfloat16),
                pltpu.VMEM((n_dev, tok, hid), jnp.bfloat16),
                pltpu.VMEM((n_dev, 8, 128), jnp.float32),
                pltpu.VMEM((n_local, HALF, ffn), jnp.bfloat16),
                pltpu.VMEM((9, tok, hid), jnp.float32),
                pltpu.VMEM((7, tok, hid), jnp.float32),
                pltpu.VMEM((2, HALF, hid), jnp.float32),
                dma((5,)), dma((16,)), dma((16,)), dma((3, 7)), dma((3, 7)), dma((8, 3)), dma((8, 3)),
                dma((3, 7)), dma((3, 7)), dma((2,)), dma((2,)), pltpu.SemaphoreType.REGULAR((2,)),
            ],
            compiler_params=pltpu.CompilerParams(collective_id=0, has_side_effects=True, vmem_limit_bytes=66_000_000),
            name='moe_kernel',
        )(x_loc, tiles, w_g, w_u, w_d)

    tok_spec = P(TOKEN_AXES, None)
    w_spec = P(EXPERT_AXES, None, None)
    return jax.shard_map(local_layer, mesh=mesh, in_specs=(tok_spec, tok_spec, tok_spec, w_spec, w_spec, w_spec), out_specs=tok_spec, check_vma=False)
```

```python
import jax
import jax.numpy as jnp
from jax import lax
from jax.experimental import pallas as pl
from jax.experimental.pallas import tpu as pltpu
from jax.sharding import PartitionSpec as P

TOKEN_AXES = ('ez', 'ey', 'ex')
EXPERT_AXES = ('ex', 'ey', 'ez')
MESH = pl.DeviceIdType.MESH

ORDERS = ((2, 4, 8), (4, 8, 2), (8, 2, 4))
MASKS = tuple((0, a, b, c, a ^ b, a ^ c, b ^ c, 14) for a, b, c in ORDERS)
COUNTS = (176, 176, 160)
STARTS = (0, 176, 352)
GATHER = ((0, 0), (0, 1), (0, 2), (1, 1), (1, 2), (2, 2), (4, 2))
ONWARD = {0: (3, 4), 1: (5,), 2: (), 3: (6,), 4: (), 5: (), 6: ()}
REDUCE = ((1, 0, 0), (4, 2, 0), (7, 6, 0), (5, 3, 0), (6, 3, 1), (2, 0, 1), (3, 0, 2))
BITS = (2, 4, 8, 1)
PATHS = {m: [b for b in BITS if m & b] for m in range(16)}
TILE_MOVES = (
    [(0, m) for m in range(1, 16)],
    [(1, m) for m in range(16) if len(PATHS[m]) > 1],
    [(2, m) for m in (7, 11, 13)],
    [(2, m) for m in (14, 15)],
    [(3, 15)],
)
HALF = 256
QUARTER = 128


def peer(mask):
    z, y, e = lax.axis_index('ez'), lax.axis_index('ey'), lax.axis_index('ex')
    x, c = e // 2, e % 2
    z = 1 - z if mask & 8 else z
    y = 1 - y if mask & 4 else y
    x = 1 - x if mask & 2 else x
    c = 1 - c if mask & 1 else c
    return z, y, 2 * x + c


def moe_kernel(x_hbm, ids_hbm, gates_hbm, w1_hbm, w3_hbm, w2_hbm, sum_hbm, last_hbm,
               w1, w3, w2, ids, gates, x_all, tiles, merged, act, acc, rs, dd_out, dd_in,
               load_sem, gt_send, gt_recv, ag_send, ag_recv, xd_send, xd_recv,
               rs_send, rs_recv, dd_send, dd_recv, dd_free):
    tok = x_hbm.shape[0]

    def remote(src, dst, ssem, rsem, mask):
        return pltpu.make_async_remote_copy(src, dst, ssem, rsem, device_id=peer(mask), device_id_type=MESH)

    def drain(ref, sem):
        pltpu.make_async_copy(ref, ref, sem).wait()

    def part(p):
        return pl.ds(STARTS[p], COUNTS[p])

    def gather_start(k):
        w, a = GATHER[k]
        for p in range(3):
            remote(x_all.at[2 * w, part(p)], x_all.at[2 * (k + 1), part(p)], ag_send, ag_recv.at[k], ORDERS[p][a]).start()

    def gather_wait(k):
        drain(x_all.at[2 * (k + 1)], ag_recv.at[k])

    def pair_copy(w):
        return remote(x_all.at[2 * w], x_all.at[2 * w + 1], xd_send, xd_recv.at[w], 1)

    def reduce_start(k):
        w, _, a = REDUCE[k]
        for p in range(3):
            dst = last_hbm.at[part(p)] if k == 6 else rs.at[k, part(p)]
            remote(acc.at[w, part(p)], dst, rs_send, rs_recv.at[k], ORDERS[p][a]).start()

    def reduce_wait(k):
        drain(acc.at[0], rs_recv.at[k])

    def partial_copy(s):
        return remote(dd_out.at[s], dd_in.at[s], dd_send.at[s], dd_recv.at[s], 1)

    def tiles_start(g):
        for hop, m in TILE_MOVES[g]:
            remote(tiles.at[hop, m], tiles.at[hop + 1, m], gt_send, gt_recv.at[g], PATHS[m][hop]).start()

    def tiles_wait(g):
        drain(tiles.at[0, pl.ds(0, len(TILE_MOVES[g]))], gt_recv.at[g])

    x_load = pltpu.make_async_copy(x_hbm, x_all.at[0], load_sem.at[0])
    loads = [pltpu.make_async_copy(s, d, load_sem.at[1 + i]) for i, (s, d) in enumerate((
        (ids_hbm, ids), (gates_hbm, gates), (w1_hbm, w1), (w3_hbm, w3), (w2_hbm, w2)))]

    barrier = pltpu.get_barrier_semaphore()
    for mask in BITS:
        pl.semaphore_signal(barrier, inc=1, device_id=peer(mask), device_id_type=MESH)
    x_load.start()
    for c in loads:
        c.start()
    for c in loads[:2]:
        c.wait()
    for m in range(16):
        z, y, e = peer(m)
        for l in range(2):
            hit = ids[...] == 2 * (e * 4 + y * 2 + z) + l
            row = jnp.sum(jnp.where(hit, gates[...], 0.0), axis=0, keepdims=True)
            for q in range(4):
                tiles[0, m, pl.ds(2 * q + l, 1), :] = row[:, q * QUARTER:(q + 1) * QUARTER]
    x_load.wait()
    pl.semaphore_wait(barrier, 4)
    tiles_start(0)
    gather_start(0)
    pair_copy(0).start()
    tiles_wait(0)
    tiles_start(1)
    gather_start(1)
    gather_start(2)
    for c in loads[2:]:
        c.wait()

    def merge_tiles(w):
        token = lax.broadcasted_iota(jnp.int32, (8, QUARTER), 0) // 2 * QUARTER + lax.broadcasted_iota(jnp.int32, (8, QUARTER), 1)
        for side in range(2):
            t = [tiles[len(PATHS[MASKS[p][w] | side]), MASKS[p][w] | side] for p in range(3)]
            merged[2 * w + side] = jnp.where(token < STARTS[1], t[0], jnp.where(token < STARTS[2], t[1], t[2]))

    def before(j):
        if j % 2 == 1 and j < 14:
            w = (j + 1) // 2
            gather_wait(w - 1)
            for k in ONWARD[w - 1]:
                gather_start(k)
            pair_copy(w).start()
        if j == 1:
            tiles_wait(1)
            tiles_start(2)
            tiles_start(3)
        if j == 8:
            tiles_wait(2)
        if j == 13:
            tiles_wait(3)
            tiles_start(4)
        if j == 14:
            tiles_wait(4)
        if j % 2 == 0 and j < 16:
            merge_tiles(j // 2)
            pair_copy(j // 2).wait_recv()

    def after(j):
        if j == 7:
            reduce_start(0)
        if j == 10:
            reduce_start(1)

    def up(slot, rows):
        for l in range(2):
            for n in range(2):
                cs = slice(n * 256, n * 256 + 256)
                x_in = x_all[slot, rows, :]
                h1 = jnp.dot(x_in, w1[l, :, cs], preferred_element_type=jnp.float32)
                h3 = jnp.dot(x_in, w3[l, :, cs], preferred_element_type=jnp.float32)
                act[l, :, cs] = (h1 * jax.nn.sigmoid(h1) * h3).astype(jnp.bfloat16)

    def down(slot, h, store):
        columns = merged[slot].T
        gate = []
        for l in range(2):
            halves = [jnp.where(h == 0, columns[:, 2 * i + l:2 * i + l + 1], columns[:, 4 + 2 * i + l:5 + 2 * i + l]) for i in range(2)]
            gate.append(jnp.concatenate(halves, axis=0))
        for n in range(4):
            cs = slice(n * 256, n * 256 + 256)
            total = None
            for l in range(2):
                o = jnp.dot(act[l], w2[l, :, cs], preferred_element_type=jnp.float32)
                o = o.astype(jnp.bfloat16).astype(jnp.float32)
                term = jnp.where(gate[l] > 0, gate[l] * o, 0.0)
                total = term if total is None else total + term
            store(cs, total)

    @pl.loop(0, 17)
    def _(i):
        for j in range(16):
            @pl.when(i == j)
            def _(j=j):
                before(j)

        @pl.when(i < 16)
        def _():
            w, h = i // 2, i % 2
            rows = pl.ds(pl.multiple_of(h * HALF, HALF), HALF)

            @pl.when(i >= 2)
            def _():
                partial_copy(h).wait_send()

            up(2 * w + 1, rows)

            def store(cs, total):
                dd_out[h, :, cs] = total

            down(2 * w + 1, h, store)

            @pl.when(i >= 2)
            def _():
                pl.semaphore_wait(dd_free.at[h], 1)

            partial_copy(h).start()

        @pl.when(i > 0)
        def _():
            w, h = (i - 1) // 2, (i - 1) % 2
            rows = pl.ds(pl.multiple_of(h * HALF, HALF), HALF)
            up(2 * w, rows)
            partial_copy(h).wait_recv()

            def store(cs, total):
                acc[w, rows, cs] = total + dd_in[h, :, cs]

            down(2 * w, h, store)

            @pl.when(i < 15)
            def _():
                pl.semaphore_signal(dd_free.at[h], inc=1, device_id=peer(1), device_id_type=MESH)

        for j in (7, 10):
            @pl.when(i == j)
            def _(j=j):
                after(j)

    reduce_start(2)
    reduce_start(3)

    def add(k):
        _, w, _ = REDUCE[k]
        reduce_wait(k)

        @pl.loop(0, tok // 16)
        def _(i):
            rows = pl.ds(pl.multiple_of(i * 16, 16), 16)
            got = acc[w, rows, :] + rs[k, rows, :]
            if k == 5:
                got = got + x_all[0, rows, :].astype(jnp.float32)
            acc[w, rows, :] = got

    add(0)
    add(1)
    add(2)
    reduce_start(4)
    reduce_start(5)
    add(3)
    add(4)
    reduce_start(6)
    add(5)
    store = pltpu.make_async_copy(acc.at[0], sum_hbm, load_sem.at[0])
    store.start()

    drain(tiles.at[pl.ds(0, 2)], gt_send)
    drain(x_all.at[pl.ds(0, 7)], ag_send)
    drain(x_all.at[pl.ds(0, 8)], xd_send)
    for h in range(2):
        partial_copy(h).wait_send()
    store.wait()
    drain(acc.at[pl.ds(0, 7)], rs_send)
    reduce_wait(6)


def final_kernel(a_hbm, b_hbm, y_hbm, a, b, y, in_sem, out_sem):
    n = in_sem.shape[0]
    rows = a.shape[0] // n
    loads, stores = [], []
    for c in range(n):
        part = pl.ds(c * rows, rows)
        loads.append([pltpu.make_async_copy(s.at[part], d.at[part], in_sem.at[c, i]) for i, (s, d) in enumerate(((a_hbm, a), (b_hbm, b)))])
        stores.append(pltpu.make_async_copy(y.at[part], y_hbm.at[part], out_sem.at[c]))
        for copy in loads[c]:
            copy.start()
    for c in range(n):
        for copy in loads[c]:
            copy.wait()

        @pl.loop(0, rows // 16)
        def _(i):
            at = pl.ds(pl.multiple_of(c * rows + i * 16, 16), 16)
            y[at, :] = (a[at, :] + b[at, :]).astype(y.dtype)

        stores[c].start()
    for copy in stores:
        copy.wait()


def solution(mesh):
    n_dev = mesh.shape['ez'] * mesh.shape['ey'] * mesh.shape['ex']

    def local_layer(x_loc, ids_loc, gates_loc, w_g, w_u, w_d):
        tok, hid = x_loc.shape
        top_k = ids_loc.shape[1]
        n_local, _, ffn = w_g.shape
        hbm = pl.BlockSpec(memory_space=pl.ANY)
        dma = pltpu.SemaphoreType.DMA
        f32, bf16 = jnp.float32, jnp.bfloat16
        total, last = pl.pallas_call(
            moe_kernel,
            out_shape=[jax.ShapeDtypeStruct((tok, hid), f32)] * 2,
            in_specs=[hbm] * 6,
            out_specs=[hbm] * 2,
            scratch_shapes=[
                pltpu.VMEM((n_local, hid, ffn), bf16),
                pltpu.VMEM((n_local, hid, ffn), bf16),
                pltpu.VMEM((n_local, ffn, hid), bf16),
                pltpu.VMEM((top_k, tok), jnp.int32),
                pltpu.VMEM((top_k, tok), f32),
                pltpu.VMEM((n_dev, tok, hid), bf16),
                pltpu.VMEM((5, n_dev, 8, QUARTER), f32),
                pltpu.VMEM((n_dev, 8, QUARTER), f32),
                pltpu.VMEM((n_local, HALF, ffn), bf16),
                pltpu.VMEM((8, tok, hid), f32),
                pltpu.VMEM((6, tok, hid), f32),
                pltpu.VMEM((2, HALF, hid), f32),
                pltpu.VMEM((2, HALF, hid), f32),
                dma((6,)), dma, dma((5,)), dma, dma((7,)), dma, dma((8,)),
                dma, dma((7,)), dma((2,)), dma((2,)), pltpu.SemaphoreType.REGULAR((2,)),
            ],
            compiler_params=pltpu.CompilerParams(collective_id=0, has_side_effects=True, vmem_limit_bytes=66_000_000),
            name='moe_kernel',
        )(x_loc, ids_loc.T, gates_loc.T, w_g, w_u, w_d)
        return pl.pallas_call(
            final_kernel,
            out_shape=jax.ShapeDtypeStruct((tok, hid), bf16),
            in_specs=[hbm] * 2,
            out_specs=hbm,
            scratch_shapes=[pltpu.VMEM((tok, hid), f32), pltpu.VMEM((tok, hid), f32), pltpu.VMEM((tok, hid), bf16), dma((4, 2)), dma((4,))],
            name='final_kernel',
        )(total, last)

    tok_spec = P(TOKEN_AXES, None)
    w_spec = P(EXPERT_AXES, None, None)
    return jax.shard_map(local_layer, mesh=mesh, in_specs=(tok_spec, tok_spec, tok_spec, w_spec, w_spec, w_spec), out_specs=tok_spec, check_vma=False)
```

```python
import jax
import jax.numpy as jnp
from jax import lax
from jax.experimental import pallas as pl
from jax.experimental.pallas import tpu as pltpu
from jax.sharding import PartitionSpec as P

TOKEN_AXES = ('ez', 'ey', 'ex')
EXPERT_AXES = ('ex', 'ey', 'ez')
MESH = pl.DeviceIdType.MESH

PARTS = (
    (0, 160, (2, 4, 8), (2, 4, 8)),
    (160, 160, (4, 8, 2), (4, 8, 2)),
    (320, 160, (8, 2, 4), (8, 2, 4)),
    (480, 16, (2, 4, 8), (2, 8, 4)),
    (496, 16, (2, 4, 8), (4, 2, 8)),
)
GATHER = ((0, 0), (0, 1), (0, 2), (1, 1), (1, 2), (2, 2), (4, 2))
ONWARD = {0: (3, 4), 1: (5,), 2: (), 3: (6,), 4: (), 5: (), 6: ()}


def masks(part):
    a, b, c = part[2]
    return 0, a, b, c, a ^ b, a ^ c, b ^ c, 14


def reduce_move(part, k):
    a, b, c = part[3]
    mask, axis = ((a, a), (a ^ b, a), (14, a), (a ^ c, a), (b ^ c, b), (b, b), (c, c))[k]
    return masks(part).index(mask), masks(part).index(mask ^ axis), axis


FIRST = [(r, 128, part) for part in PARTS[:3] for r in part[:1]]
SECOND = [(part[0] + 128, 32, part) for part in PARTS[:3]] + [(part[0], part[1], part) for part in PARTS[3:]]
SECOND_AT = (0, 32, 64, 96, 112)
SECOND_ROWS = 128
BITS = (2, 4, 8, 1)
PATHS = {m: [b for b in BITS if m & b] for m in range(16)}
TILE_MOVES = (
    [(0, m) for m in range(1, 16)],
    [(1, m) for m in range(16) if len(PATHS[m]) > 1],
    [(2, m) for m in (7, 11, 13)],
    [(2, m) for m in (14, 15)],
    [(3, 15)],
)
HALF = 256
QUARTER = 128


def peer(mask):
    z, y, e = lax.axis_index('ez'), lax.axis_index('ey'), lax.axis_index('ex')
    x, c = e // 2, e % 2
    z = 1 - z if mask & 8 else z
    y = 1 - y if mask & 4 else y
    x = 1 - x if mask & 2 else x
    c = 1 - c if mask & 1 else c
    return z, y, 2 * x + c


def moe_kernel(x_hbm, ids_hbm, gates_hbm, w1_hbm, w3_hbm, w2_hbm, y_hbm, sum_hbm, last_hbm,
               w1, w3, w2, ids, gates, x_all, tiles, merged, act, acc, rs, dd_out, dd_in,
               load_sem, gt_send, gt_recv, ag_send, ag_recv, xd_send, xd_recv,
               rs_send, rs_recv, dd_send, dd_recv, dd_free):
    tok = x_hbm.shape[0]

    def remote(src, dst, ssem, rsem, mask):
        return pltpu.make_async_remote_copy(src, dst, ssem, rsem, device_id=peer(mask), device_id_type=MESH)

    def drain(ref, sem):
        pltpu.make_async_copy(ref, ref, sem).wait()

    def gather_start(k):
        w, a = GATHER[k]
        for part in PARTS:
            rows = pl.ds(part[0], part[1])
            remote(x_all.at[2 * w, rows], x_all.at[2 * (k + 1), rows], ag_send, ag_recv.at[k], part[2][a]).start()

    def gather_wait(k):
        drain(x_all.at[2 * (k + 1)], ag_recv.at[k])

    def pair_copy(w):
        return remote(x_all.at[2 * w], x_all.at[2 * w + 1], xd_send, xd_recv.at[w], 1)

    def reduce_start(k, parts=PARTS):
        for part in parts:
            w, _, axis = reduce_move(part, k)
            rows = pl.ds(part[0], part[1])
            remote(acc.at[w, rows], rs.at[k, rows], rs_send, rs_recv.at[k], axis).start()

    def reduce_last_start():
        for r, n, part in FIRST:
            w, _, axis = reduce_move(part, 6)
            remote(acc.at[w, pl.ds(r, n)], rs.at[6, pl.ds(r, n)], rs_send, rs_recv.at[6], axis).start()
        for at, (r, n, part) in zip(SECOND_AT, SECOND):
            w, _, axis = reduce_move(part, 6)
            remote(acc.at[w, pl.ds(r, n)], last_hbm.at[pl.ds(at, n)], rs_send, rs_recv.at[7], axis).start()

    def reduce_wait(k):
        rows = tok if k < 6 else SECOND_ROWS if k == 7 else tok - SECOND_ROWS
        drain(acc.at[0, pl.ds(0, rows)], rs_recv.at[k])

    def partial_copy(s):
        return remote(dd_out.at[s], dd_in.at[s], dd_send.at[s], dd_recv.at[s], 1)

    def tiles_start(g):
        for hop, m in TILE_MOVES[g]:
            remote(tiles.at[hop, m], tiles.at[hop + 1, m], gt_send, gt_recv.at[g], PATHS[m][hop]).start()

    def tiles_wait(g):
        drain(tiles.at[0, pl.ds(0, len(TILE_MOVES[g]))], gt_recv.at[g])

    x_load = pltpu.make_async_copy(x_hbm, x_all.at[0], load_sem.at[0])
    loads = [pltpu.make_async_copy(s, d, load_sem.at[1 + i]) for i, (s, d) in enumerate((
        (ids_hbm, ids), (gates_hbm, gates), (w1_hbm, w1), (w3_hbm, w3), (w2_hbm, w2)))]

    barrier = pltpu.get_barrier_semaphore()
    for mask in BITS:
        pl.semaphore_signal(barrier, inc=1, device_id=peer(mask), device_id_type=MESH)
    x_load.start()
    for c in loads:
        c.start()
    for c in loads[:2]:
        c.wait()
    for m in range(16):
        z, y, e = peer(m)
        for l in range(2):
            hit = ids[...] == 2 * (e * 4 + y * 2 + z) + l
            row = jnp.sum(jnp.where(hit, gates[...], 0.0), axis=0, keepdims=True)
            for q in range(4):
                tiles[0, m, pl.ds(2 * q + l, 1), :] = row[:, q * QUARTER:(q + 1) * QUARTER]
    x_load.wait()
    pl.semaphore_wait(barrier, 4)
    tiles_start(0)
    gather_start(0)
    pair_copy(0).start()
    tiles_wait(0)
    tiles_start(1)
    gather_start(1)
    gather_start(2)
    for c in loads[2:]:
        c.wait()

    def merge_tiles(w):
        token = lax.broadcasted_iota(jnp.int32, (8, QUARTER), 0) // 2 * QUARTER + lax.broadcasted_iota(jnp.int32, (8, QUARTER), 1)
        for side in range(2):
            tile = None
            for part in PARTS:
                m = masks(part)[w] | side
                mine = tiles[len(PATHS[m]), m]
                tile = mine if tile is None else jnp.where(token < part[0], tile, mine)
            merged[2 * w + side] = tile

    def before(j):
        if j % 2 == 1 and j < 14:
            w = (j + 1) // 2
            gather_wait(w - 1)
            for k in ONWARD[w - 1]:
                gather_start(k)
            pair_copy(w).start()
        if j == 1:
            tiles_wait(1)
            tiles_start(2)
            tiles_start(3)
        if j == 8:
            tiles_wait(2)
        if j == 13:
            tiles_wait(3)
            tiles_start(4)
        if j == 14:
            tiles_wait(4)
        if j % 2 == 0 and j < 16:
            merge_tiles(j // 2)
            pair_copy(j // 2).wait_recv()

    def after(j):
        if j == 7:
            reduce_start(0)
        if j == 10:
            reduce_start(1, PARTS[:3])

    def up(slot, rows):
        for l in range(2):
            for n in range(2):
                cs = slice(n * 256, n * 256 + 256)
                x_in = x_all[slot, rows, :]
                h1 = jnp.dot(x_in, w1[l, :, cs], preferred_element_type=jnp.float32)
                h3 = jnp.dot(x_in, w3[l, :, cs], preferred_element_type=jnp.float32)
                act[l, :, cs] = (h1 * jax.nn.sigmoid(h1) * h3).astype(jnp.bfloat16)

    def down(slot, h, store):
        columns = merged[slot].T
        gate = []
        for l in range(2):
            halves = [jnp.where(h == 0, columns[:, 2 * i + l:2 * i + l + 1], columns[:, 4 + 2 * i + l:5 + 2 * i + l]) for i in range(2)]
            gate.append(jnp.concatenate(halves, axis=0))
        for n in range(4):
            cs = slice(n * 256, n * 256 + 256)
            total = None
            for l in range(2):
                o = jnp.dot(act[l], w2[l, :, cs], preferred_element_type=jnp.float32)
                o = o.astype(jnp.bfloat16).astype(jnp.float32)
                term = jnp.where(gate[l] > 0, gate[l] * o, 0.0)
                total = term if total is None else total + term
            store(cs, total)

    @pl.loop(0, 17)
    def _(i):
        for j in range(16):
            @pl.when(i == j)
            def _(j=j):
                before(j)

        @pl.when(i < 16)
        def _():
            w, h = i // 2, i % 2
            rows = pl.ds(pl.multiple_of(h * HALF, HALF), HALF)

            @pl.when(i >= 2)
            def _():
                partial_copy(h).wait_send()

            up(2 * w + 1, rows)

            def store(cs, total):
                dd_out[h, :, cs] = total

            down(2 * w + 1, h, store)

            @pl.when(i >= 2)
            def _():
                pl.semaphore_wait(dd_free.at[h], 1)

            partial_copy(h).start()

        @pl.when(i > 0)
        def _():
            w, h = (i - 1) // 2, (i - 1) % 2
            rows = pl.ds(pl.multiple_of(h * HALF, HALF), HALF)
            up(2 * w, rows)
            partial_copy(h).wait_recv()

            def store(cs, total):
                acc[w, rows, cs] = total + dd_in[h, :, cs]

            down(2 * w, h, store)

            @pl.when(i < 15)
            def _():
                pl.semaphore_signal(dd_free.at[h], inc=1, device_id=peer(1), device_id_type=MESH)

        for j in (7, 10):
            @pl.when(i == j)
            def _(j=j):
                after(j)

    reduce_start(1, PARTS[3:])
    reduce_start(2)
    reduce_start(3)

    def sum_rows(first, n, fn):
        @pl.loop(0, n // 16)
        def _(i):
            fn(pl.ds(pl.multiple_of(first + i * 16, 16), 16))

    def add(k):
        reduce_wait(k)
        for first, n, part in ((0, 480, PARTS[0]), (480, 16, PARTS[3]), (496, 16, PARTS[4])):
            w = reduce_move(part, k)[1]

            def one(rows, w=w):
                got = acc[w, rows, :] + rs[k, rows, :]
                if k == 5:
                    got = got + x_all[0, rows, :].astype(jnp.float32)
                acc[w, rows, :] = got

            sum_rows(first, n, one)

    add(0)
    add(1)
    add(2)
    reduce_start(4)
    reduce_start(5)
    add(3)
    add(4)
    reduce_last_start()
    add(5)
    stores = [pltpu.make_async_copy(acc.at[0, pl.ds(r, n)], sum_hbm.at[pl.ds(at, n)], load_sem.at[i])
              for i, (at, (r, n, _)) in enumerate(zip(SECOND_AT, SECOND))]
    for c in stores:
        c.start()

    drain(tiles.at[pl.ds(0, 2)], gt_send)
    drain(x_all.at[pl.ds(0, 7)], ag_send)
    drain(x_all.at[pl.ds(0, 8)], xd_send)
    for h in range(2):
        partial_copy(h).wait_send()
    for c in stores:
        c.wait()

    reduce_wait(6)
    stores = []
    for i, (r, n, _) in enumerate(FIRST):
        def one(rows):
            x_all[1, rows, :] = (acc[0, rows, :] + rs[6, rows, :]).astype(x_all.dtype)

        sum_rows(r, n, one)
        stores.append(pltpu.make_async_copy(x_all.at[1, pl.ds(r, n)], y_hbm.at[pl.ds(r, n)], load_sem.at[i]))
        stores[i].start()
    for c in stores:
        c.wait()
    drain(acc.at[pl.ds(0, 7)], rs_send)
    reduce_wait(7)


def final_kernel(y_in, a_hbm, b_hbm, y_hbm, a, b, y, in_sem, out_sem):
    ab = [pltpu.make_async_copy(s, d, in_sem.at[i]) for i, (s, d) in enumerate(((a_hbm, a), (b_hbm, b)))]
    ys = [pltpu.make_async_copy(y_in.at[pl.ds(r, n)], y.at[pl.ds(r, n)], in_sem.at[2 + i]) for i, (r, n, _) in enumerate(FIRST)]
    outs = [pltpu.make_async_copy(y.at[pl.ds(r, n)], y_hbm.at[pl.ds(r, n)], out_sem.at[i]) for i, (r, n, _) in enumerate(FIRST + SECOND)]
    for c in ab + ys:
        c.start()
    for c in ab:
        c.wait()
    for i, (at, (r, n, _)) in enumerate(zip(SECOND_AT, SECOND)):
        y[pl.ds(r, n), :] = (a[pl.ds(at, n), :] + b[pl.ds(at, n), :]).astype(y.dtype)
        outs[3 + i].start()
    for i, c in enumerate(ys):
        c.wait()
        outs[i].start()
    for c in outs:
        c.wait()


def solution(mesh):
    n_dev = mesh.shape['ez'] * mesh.shape['ey'] * mesh.shape['ex']

    def local_layer(x_loc, ids_loc, gates_loc, w_g, w_u, w_d):
        tok, hid = x_loc.shape
        top_k = ids_loc.shape[1]
        n_local, _, ffn = w_g.shape
        hbm = pl.BlockSpec(memory_space=pl.ANY)
        dma = pltpu.SemaphoreType.DMA
        f32, bf16 = jnp.float32, jnp.bfloat16
        second = jax.ShapeDtypeStruct((SECOND_ROWS, hid), f32)
        first, total, last = pl.pallas_call(
            moe_kernel,
            out_shape=[jax.ShapeDtypeStruct((tok, hid), bf16), second, second],
            in_specs=[hbm] * 6,
            out_specs=[hbm] * 3,
            scratch_shapes=[
                pltpu.VMEM((n_local, hid, ffn), bf16),
                pltpu.VMEM((n_local, hid, ffn), bf16),
                pltpu.VMEM((n_local, ffn, hid), bf16),
                pltpu.VMEM((top_k, tok), jnp.int32),
                pltpu.VMEM((top_k, tok), f32),
                pltpu.VMEM((n_dev, tok, hid), bf16),
                pltpu.VMEM((5, n_dev, 8, QUARTER), f32),
                pltpu.VMEM((n_dev, 8, QUARTER), f32),
                pltpu.VMEM((n_local, HALF, ffn), bf16),
                pltpu.VMEM((8, tok, hid), f32),
                pltpu.VMEM((7, tok, hid), f32),
                pltpu.VMEM((2, HALF, hid), f32),
                pltpu.VMEM((2, HALF, hid), f32),
                dma((6,)), dma, dma((5,)), dma, dma((7,)), dma, dma((8,)),
                dma, dma((8,)), dma((2,)), dma((2,)), pltpu.SemaphoreType.REGULAR((2,)),
            ],
            compiler_params=pltpu.CompilerParams(collective_id=0, has_side_effects=True, vmem_limit_bytes=66_000_000),
            name='moe_kernel',
        )(x_loc, ids_loc.T, gates_loc.T, w_g, w_u, w_d)
        return pl.pallas_call(
            final_kernel,
            out_shape=jax.ShapeDtypeStruct((tok, hid), bf16),
            in_specs=[hbm] * 3,
            out_specs=hbm,
            scratch_shapes=[pltpu.VMEM((SECOND_ROWS, hid), f32), pltpu.VMEM((SECOND_ROWS, hid), f32), pltpu.VMEM((tok, hid), bf16), dma((5,)), dma((8,))],
            name='final_kernel',
        )(first, total, last)

    tok_spec = P(TOKEN_AXES, None)
    w_spec = P(EXPERT_AXES, None, None)
    return jax.shard_map(local_layer, mesh=mesh, in_specs=(tok_spec, tok_spec, tok_spec, w_spec, w_spec, w_spec), out_specs=tok_spec, check_vma=False)
```

```python
import jax
import jax.numpy as jnp
from jax import lax
from jax.experimental import pallas as pl
from jax.experimental.pallas import tpu as pltpu
from jax.sharding import PartitionSpec as P

TOKEN_AXES = ('ez', 'ey', 'ex')
EXPERT_AXES = ('ex', 'ey', 'ez')
MESH = pl.DeviceIdType.MESH

PARTS = (
    (0, 160, (2, 4, 8), (2, 4, 8)),
    (160, 160, (4, 8, 2), (4, 8, 2)),
    (320, 160, (8, 2, 4), (8, 2, 4)),
    (480, 16, (2, 4, 8), (2, 8, 4)),
    (496, 16, (2, 4, 8), (4, 2, 8)),
)
GATHER = ((0, 0), (0, 1), (0, 2), (1, 1), (1, 2), (2, 2), (4, 2))
ONWARD = {0: (3, 4), 1: (5,), 2: (), 3: (6,), 4: (), 5: (), 6: ()}


def masks(part):
    a, b, c = part[2]
    return 0, a, b, c, a ^ b, a ^ c, b ^ c, 14


def reduce_move(part, k):
    a, b, c = part[3]
    mask, axis = ((a, a), (a ^ b, a), (14, a), (a ^ c, a), (b ^ c, b), (b, b), (c, c))[k]
    return masks(part).index(mask), masks(part).index(mask ^ axis), axis


FIRST = [(part[0], 128, part) for part in PARTS[:3]]
SECOND = [(part[0] + 128, 32, part) for part in PARTS[:3]] + [(part[0], part[1], part) for part in PARTS[3:]]
SECOND_ROWS = 128
BITS = (2, 4, 8, 1)
PATHS = {m: [b for b in BITS if m & b] for m in range(16)}
TILE_MOVES = (
    [(0, m) for m in range(1, 16)],
    [(1, m) for m in range(16) if len(PATHS[m]) > 1],
    [(2, m) for m in (7, 11, 13)],
    [(2, m) for m in (14, 15)],
    [(3, 15)],
)
HALF = 256
QUARTER = 128


def peer(mask):
    z, y, e = lax.axis_index('ez'), lax.axis_index('ey'), lax.axis_index('ex')
    x, c = e // 2, e % 2
    z = 1 - z if mask & 8 else z
    y = 1 - y if mask & 4 else y
    x = 1 - x if mask & 2 else x
    c = 1 - c if mask & 1 else c
    return z, y, 2 * x + c


def moe_kernel(x_hbm, ids_hbm, gates_hbm, w1_hbm, w3_hbm, w2_hbm, y_out,
               w1, w3, w2, ids, gates, x_all, tiles, merged, act, acc, rs, dd_out, dd_in,
               load_sem, gt_send, gt_recv, ag_send, ag_recv, xd_send, xd_recv,
               rs_send, rs_recv, dd_send, dd_recv, dd_free):
    tok = x_hbm.shape[0]

    def remote(src, dst, ssem, rsem, mask):
        return pltpu.make_async_remote_copy(src, dst, ssem, rsem, device_id=peer(mask), device_id_type=MESH)

    def drain(ref, sem):
        pltpu.make_async_copy(ref, ref, sem).wait()

    def gather_start(k):
        w, a = GATHER[k]
        for part in PARTS:
            rows = pl.ds(part[0], part[1])
            remote(x_all.at[2 * w, rows], x_all.at[2 * (k + 1), rows], ag_send, ag_recv.at[k], part[2][a]).start()

    def gather_wait(k):
        drain(x_all.at[2 * (k + 1)], ag_recv.at[k])

    def pair_copy(w):
        return remote(x_all.at[2 * w], x_all.at[2 * w + 1], xd_send, xd_recv.at[w], 1)

    def reduce_start(k, parts=PARTS):
        for part in parts:
            w, _, axis = reduce_move(part, k)
            rows = pl.ds(part[0], part[1])
            remote(acc.at[w, rows], rs.at[k, rows], rs_send, rs_recv.at[k], axis).start()

    def reduce_last_start():
        for i, piece in enumerate((FIRST, SECOND)):
            for r, n, part in piece:
                w, _, axis = reduce_move(part, 6)
                rows = pl.ds(r, n)
                remote(acc.at[w, rows], rs.at[6, rows], rs_send, rs_recv.at[6 + i], axis).start()

    def reduce_wait(k):
        rows = tok if k < 6 else SECOND_ROWS if k == 7 else tok - SECOND_ROWS
        drain(acc.at[0, pl.ds(0, rows)], rs_recv.at[k])

    def partial_copy(s):
        return remote(dd_out.at[s], dd_in.at[s], dd_send.at[s], dd_recv.at[s], 1)

    def tiles_start(g):
        for hop, m in TILE_MOVES[g]:
            remote(tiles.at[hop, m], tiles.at[hop + 1, m], gt_send, gt_recv.at[g], PATHS[m][hop]).start()

    def tiles_wait(g):
        drain(tiles.at[0, pl.ds(0, len(TILE_MOVES[g]))], gt_recv.at[g])

    x_load = pltpu.make_async_copy(x_hbm, x_all.at[0], load_sem.at[0])
    loads = [pltpu.make_async_copy(s, d, load_sem.at[1 + i]) for i, (s, d) in enumerate((
        (ids_hbm, ids), (gates_hbm, gates), (w1_hbm, w1), (w3_hbm, w3), (w2_hbm, w2)))]

    barrier = pltpu.get_barrier_semaphore()
    for mask in BITS:
        pl.semaphore_signal(barrier, inc=1, device_id=peer(mask), device_id_type=MESH)
    x_load.start()
    for c in loads:
        c.start()
    for c in loads[:2]:
        c.wait()
    for m in range(16):
        z, y, e = peer(m)
        for l in range(2):
            hit = ids[...] == 2 * (e * 4 + y * 2 + z) + l
            row = jnp.sum(jnp.where(hit, gates[...], 0.0), axis=0, keepdims=True)
            for q in range(4):
                tiles[0, m, pl.ds(2 * q + l, 1), :] = row[:, q * QUARTER:(q + 1) * QUARTER]
    x_load.wait()
    pl.semaphore_wait(barrier, 4)
    tiles_start(0)
    gather_start(0)
    pair_copy(0).start()
    tiles_wait(0)
    tiles_start(1)
    gather_start(1)
    gather_start(2)
    for c in loads[2:]:
        c.wait()

    def merge_tiles(w):
        token = lax.broadcasted_iota(jnp.int32, (8, QUARTER), 0) // 2 * QUARTER + lax.broadcasted_iota(jnp.int32, (8, QUARTER), 1)
        for side in range(2):
            tile = None
            for part in PARTS:
                m = masks(part)[w] | side
                mine = tiles[len(PATHS[m]), m]
                tile = mine if tile is None else jnp.where(token < part[0], tile, mine)
            merged[2 * w + side] = tile

    def before(j):
        if j % 2 == 1 and j < 14:
            w = (j + 1) // 2
            gather_wait(w - 1)
            for k in ONWARD[w - 1]:
                gather_start(k)
            pair_copy(w).start()
        if j == 1:
            tiles_wait(1)
            tiles_start(2)
            tiles_start(3)
        if j == 8:
            tiles_wait(2)
        if j == 13:
            tiles_wait(3)
            tiles_start(4)
        if j == 14:
            tiles_wait(4)
        if j % 2 == 0 and j < 16:
            merge_tiles(j // 2)
            pair_copy(j // 2).wait_recv()

    def after(j):
        if j == 7:
            reduce_start(0)
        if j == 10:
            reduce_start(1, PARTS[:3])

    def up(slot, rows):
        for l in range(2):
            for n in range(2):
                cs = slice(n * 256, n * 256 + 256)
                x_in = x_all[slot, rows, :]
                h1 = jnp.dot(x_in, w1[l, :, cs], preferred_element_type=jnp.float32)
                h3 = jnp.dot(x_in, w3[l, :, cs], preferred_element_type=jnp.float32)
                act[l, :, cs] = (h1 * jax.nn.sigmoid(h1) * h3).astype(jnp.bfloat16)

    def down(slot, h, store):
        columns = merged[slot].T
        gate = []
        for l in range(2):
            halves = [jnp.where(h == 0, columns[:, 2 * i + l:2 * i + l + 1], columns[:, 4 + 2 * i + l:5 + 2 * i + l]) for i in range(2)]
            gate.append(jnp.concatenate(halves, axis=0))
        for n in range(4):
            cs = slice(n * 256, n * 256 + 256)
            total = None
            for l in range(2):
                o = jnp.dot(act[l], w2[l, :, cs], preferred_element_type=jnp.float32)
                o = o.astype(jnp.bfloat16).astype(jnp.float32)
                term = jnp.where(gate[l] > 0, gate[l] * o, 0.0)
                total = term if total is None else total + term
            store(cs, total)

    @pl.loop(0, 17)
    def _(i):
        for j in range(16):
            @pl.when(i == j)
            def _(j=j):
                before(j)

        @pl.when(i < 16)
        def _():
            w, h = i // 2, i % 2
            rows = pl.ds(pl.multiple_of(h * HALF, HALF), HALF)

            @pl.when(i >= 2)
            def _():
                partial_copy(h).wait_send()

            up(2 * w + 1, rows)

            def store(cs, total):
                dd_out[h, :, cs] = total

            down(2 * w + 1, h, store)

            @pl.when(i >= 2)
            def _():
                pl.semaphore_wait(dd_free.at[h], 1)

            partial_copy(h).start()

        @pl.when(i > 0)
        def _():
            w, h = (i - 1) // 2, (i - 1) % 2
            rows = pl.ds(pl.multiple_of(h * HALF, HALF), HALF)
            up(2 * w, rows)
            partial_copy(h).wait_recv()

            def store(cs, total):
                acc[w, rows, cs] = total + dd_in[h, :, cs]

            down(2 * w, h, store)

            @pl.when(i < 15)
            def _():
                pl.semaphore_signal(dd_free.at[h], inc=1, device_id=peer(1), device_id_type=MESH)

        for j in (7, 10):
            @pl.when(i == j)
            def _(j=j):
                after(j)

    reduce_start(1, PARTS[3:])
    reduce_start(2)
    reduce_start(3)

    def sum_rows(first, n, fn):
        @pl.loop(0, n // 16)
        def _(i):
            fn(pl.ds(pl.multiple_of(first + i * 16, 16), 16))

    def add(k):
        reduce_wait(k)
        for first, n, part in ((0, 480, PARTS[0]), (480, 16, PARTS[3]), (496, 16, PARTS[4])):
            w = reduce_move(part, k)[1]

            def one(rows, w=w):
                got = acc[w, rows, :] + rs[k, rows, :]
                if k == 5:
                    got = got + x_all[0, rows, :].astype(jnp.float32)
                acc[w, rows, :] = got

            sum_rows(first, n, one)

    add(0)
    add(1)
    add(2)
    reduce_start(4)
    reduce_start(5)
    add(3)
    add(4)
    reduce_last_start()
    add(5)

    drain(tiles.at[pl.ds(0, 2)], gt_send)
    drain(x_all.at[pl.ds(0, 7)], ag_send)
    drain(x_all.at[pl.ds(0, 8)], xd_send)
    for h in range(2):
        partial_copy(h).wait_send()

    def one(rows):
        y_out[rows, :] = (acc[0, rows, :] + rs[6, rows, :]).astype(y_out.dtype)

    reduce_wait(6)
    for r, n, _ in FIRST:
        sum_rows(r, n, one)
    drain(acc.at[pl.ds(0, 7)], rs_send)
    reduce_wait(7)
    for r, n, _ in SECOND:
        sum_rows(r, n, one)


def solution(mesh):
    n_dev = mesh.shape['ez'] * mesh.shape['ey'] * mesh.shape['ex']

    def local_layer(x_loc, ids_loc, gates_loc, w_g, w_u, w_d):
        tok, hid = x_loc.shape
        top_k = ids_loc.shape[1]
        n_local, _, ffn = w_g.shape
        hbm = pl.BlockSpec(memory_space=pl.ANY)
        dma = pltpu.SemaphoreType.DMA
        f32, bf16 = jnp.float32, jnp.bfloat16
        y = pl.pallas_call(
            moe_kernel,
            out_shape=pltpu.VMEM((tok, hid), bf16),
            in_specs=[hbm] * 6,
            out_specs=pl.BlockSpec(memory_space=pltpu.VMEM),
            scratch_shapes=[
                pltpu.VMEM((n_local, hid, ffn), bf16),
                pltpu.VMEM((n_local, hid, ffn), bf16),
                pltpu.VMEM((n_local, ffn, hid), bf16),
                pltpu.VMEM((top_k, tok), jnp.int32),
                pltpu.VMEM((top_k, tok), f32),
                pltpu.VMEM((n_dev, tok, hid), bf16),
                pltpu.VMEM((5, n_dev, 8, QUARTER), f32),
                pltpu.VMEM((n_dev, 8, QUARTER), f32),
                pltpu.VMEM((n_local, HALF, ffn), bf16),
                pltpu.VMEM((8, tok, hid), f32),
                pltpu.VMEM((7, tok, hid), f32),
                pltpu.VMEM((2, HALF, hid), f32),
                pltpu.VMEM((2, HALF, hid), f32),
                dma((6,)), dma, dma((5,)), dma, dma((7,)), dma, dma((8,)),
                dma, dma((8,)), dma((2,)), dma((2,)), pltpu.SemaphoreType.REGULAR((2,)),
            ],
            compiler_params=pltpu.CompilerParams(collective_id=0, has_side_effects=True, vmem_limit_bytes=62_000_000),
            name='moe_kernel',
        )(x_loc, ids_loc.T, gates_loc.T, w_g, w_u, w_d)
        return y

    tok_spec = P(TOKEN_AXES, None)
    w_spec = P(EXPERT_AXES, None, None)
    return jax.shard_map(local_layer, mesh=mesh, in_specs=(tok_spec, tok_spec, tok_spec, w_spec, w_spec, w_spec), out_specs=tok_spec, check_vma=False)
```

```python
import jax
import jax.numpy as jnp
from jax import lax
from jax.experimental import pallas as pl
from jax.experimental.pallas import tpu as pltpu
from jax.sharding import PartitionSpec as P

TOKEN_AXES = ('ez', 'ey', 'ex')
EXPERT_AXES = ('ex', 'ey', 'ez')
MESH = pl.DeviceIdType.MESH

PARTS = (
    (0, 160, (2, 4, 8), (2, 4, 8)),
    (160, 160, (4, 8, 2), (4, 8, 2)),
    (320, 160, (8, 2, 4), (8, 2, 4)),
    (480, 16, (2, 4, 8), (2, 8, 4)),
    (496, 16, (2, 4, 8), (4, 2, 8)),
)
GATHER = ((0, 0), (0, 1), (0, 2), (1, 1), (1, 2), (2, 2), (4, 2))
ONWARD = {0: (3, 4), 1: (5,), 2: (), 3: (6,), 4: (), 5: (), 6: ()}


def masks(part):
    a, b, c = part[2]
    return 0, a, b, c, a ^ b, a ^ c, b ^ c, 14


def reduce_move(part, k):
    a, b, c = part[3]
    mask, axis = ((a, a), (a ^ b, a), (14, a), (a ^ c, a), (b ^ c, b), (b, b), (c, c))[k]
    return masks(part).index(mask), masks(part).index(mask ^ axis), axis


FIRST = [(part[0], 128, part) for part in PARTS[:3]]
SECOND = [(part[0] + 128, 32, part) for part in PARTS[:3]] + [(part[0], part[1], part) for part in PARTS[3:]]
SECOND_ROWS = 128
BITS = (2, 4, 8, 1)
PATHS = {m: [b for b in BITS if m & b] for m in range(16)}
TILE_MOVES = (
    [(0, m) for m in range(1, 16)],
    [(1, m) for m in range(16) if len(PATHS[m]) > 1],
    [(2, m) for m in (7, 11, 13)],
    [(2, m) for m in (14, 15)],
    [(3, 15)],
)
HALF = 256
QUARTER = 128


def peer(mask):
    z, y, e = lax.axis_index('ez'), lax.axis_index('ey'), lax.axis_index('ex')
    x, c = e // 2, e % 2
    z = 1 - z if mask & 8 else z
    y = 1 - y if mask & 4 else y
    x = 1 - x if mask & 2 else x
    c = 1 - c if mask & 1 else c
    return z, y, 2 * x + c


def moe_kernel(x_hbm, ids_hbm, gates_hbm, w1_hbm, w3_hbm, w2_hbm, y_out,
               w1, w3, w2, ids, gates, x_all, tiles, merged, act, acc, rs, dd_out, dd_in,
               load_sem, gt_send, gt_recv, ag_send, ag_recv, xd_send, xd_recv,
               rs_send, rs_recv, dd_send, dd_recv, dd_free):
    tok = x_hbm.shape[0]

    def remote(src, dst, ssem, rsem, mask):
        return pltpu.make_async_remote_copy(src, dst, ssem, rsem, device_id=peer(mask), device_id_type=MESH)

    def drain(ref, sem):
        pltpu.make_async_copy(ref, ref, sem).wait()

    def gather_start(k):
        w, a = GATHER[k]
        for part in PARTS:
            rows = pl.ds(part[0], part[1])
            remote(x_all.at[2 * w, rows], x_all.at[2 * (k + 1), rows], ag_send, ag_recv.at[k], part[2][a]).start()

    def gather_wait(k):
        drain(x_all.at[2 * (k + 1)], ag_recv.at[k])

    def pair_copy(w):
        return remote(x_all.at[2 * w], x_all.at[2 * w + 1], xd_send, xd_recv.at[w], 1)

    def reduce_start(k, parts=PARTS):
        for part in parts:
            w, _, axis = reduce_move(part, k)
            rows = pl.ds(part[0], part[1])
            remote(acc.at[w, rows], rs.at[k, rows], rs_send, rs_recv.at[k], axis).start()

    def reduce_last_start():
        for i, piece in enumerate((FIRST, SECOND)):
            for r, n, part in piece:
                w, _, axis = reduce_move(part, 6)
                rows = pl.ds(r, n)
                remote(acc.at[w, rows], rs.at[6, rows], rs_send, rs_recv.at[6 + i], axis).start()

    def reduce_wait(k):
        rows = tok if k < 6 else SECOND_ROWS if k == 7 else tok - SECOND_ROWS
        drain(acc.at[0, pl.ds(0, rows)], rs_recv.at[k])

    def partial_copy(s):
        return remote(dd_out.at[s], dd_in.at[s], dd_send.at[s], dd_recv.at[s], 1)

    def tiles_start(g):
        for hop, m in TILE_MOVES[g]:
            remote(tiles.at[hop, m], tiles.at[hop + 1, m], gt_send, gt_recv.at[g], PATHS[m][hop]).start()

    def tiles_wait(g):
        drain(tiles.at[0, pl.ds(0, len(TILE_MOVES[g]))], gt_recv.at[g])

    x_load = pltpu.make_async_copy(x_hbm, x_all.at[0], load_sem.at[0])
    loads = [pltpu.make_async_copy(s, d, load_sem.at[1 + i]) for i, (s, d) in enumerate((
        (ids_hbm, ids), (gates_hbm, gates), (w1_hbm, w1), (w3_hbm, w3), (w2_hbm, w2)))]

    barrier = pltpu.get_barrier_semaphore()
    for mask in BITS:
        pl.semaphore_signal(barrier, inc=1, device_id=peer(mask), device_id_type=MESH)
    x_load.start()
    for c in loads:
        c.start()
    for c in loads[:2]:
        c.wait()
    for m in range(16):
        z, y, e = peer(m)
        for l in range(2):
            hit = ids[...] == 2 * (e * 4 + y * 2 + z) + l
            row = jnp.sum(jnp.where(hit, gates[...], 0.0), axis=0, keepdims=True)
            for q in range(4):
                tiles[0, m, pl.ds(2 * q + l, 1), :] = row[:, q * QUARTER:(q + 1) * QUARTER]
    x_load.wait()
    pl.semaphore_wait(barrier, 4)
    tiles_start(0)
    gather_start(0)
    pair_copy(0).start()
    tiles_wait(0)
    tiles_start(1)
    gather_start(1)
    gather_start(2)
    for c in loads[2:]:
        c.wait()

    def merge_tiles(w):
        token = lax.broadcasted_iota(jnp.int32, (8, QUARTER), 0) // 2 * QUARTER + lax.broadcasted_iota(jnp.int32, (8, QUARTER), 1)
        for side in range(2):
            tile = None
            for part in PARTS:
                m = masks(part)[w] | side
                mine = tiles[len(PATHS[m]), m]
                tile = mine if tile is None else jnp.where(token < part[0], tile, mine)
            merged[2 * w + side] = tile

    def before(j):
        if j % 2 == 1 and j < 14:
            w = (j + 1) // 2
            gather_wait(w - 1)
            for k in ONWARD[w - 1]:
                gather_start(k)
            pair_copy(w).start()
        if j == 1:
            tiles_wait(1)
            tiles_start(2)
            tiles_start(3)
        if j == 8:
            tiles_wait(2)
        if j == 13:
            tiles_wait(3)
            tiles_start(4)
        if j == 14:
            tiles_wait(4)
        if j % 2 == 0 and j < 16:
            merge_tiles(j // 2)
            pair_copy(j // 2).wait_recv()

    def after(j):
        if j == 7:
            reduce_start(0)
        if j == 10:
            reduce_start(1, PARTS[:3])

    def up(slot, rows):
        for l in range(2):
            for n in range(2):
                cs = slice(n * 256, n * 256 + 256)
                x_in = x_all[slot, rows, :]
                h1 = jnp.dot(x_in, w1[l, :, cs], preferred_element_type=jnp.float32)
                h3 = jnp.dot(x_in, w3[l, :, cs], preferred_element_type=jnp.float32)
                act[l, :, cs] = (h1 * jax.nn.sigmoid(h1) * h3).astype(jnp.bfloat16)

    def down(slot, h, store):
        columns = merged[slot].T
        gate = []
        for l in range(2):
            halves = [jnp.where(h == 0, columns[:, 2 * i + l:2 * i + l + 1], columns[:, 4 + 2 * i + l:5 + 2 * i + l]) for i in range(2)]
            gate.append(jnp.concatenate(halves, axis=0))
        for n in range(4):
            cs = slice(n * 256, n * 256 + 256)
            total = None
            for l in range(2):
                o = jnp.dot(act[l], w2[l, :, cs], preferred_element_type=jnp.float32)
                o = o.astype(jnp.bfloat16).astype(jnp.float32)
                term = jnp.where(gate[l] > 0, gate[l] * o, 0.0)
                total = term if total is None else total + term
            store(cs, total)

    @pl.loop(0, 17)
    def _(i):
        for j in range(16):
            @pl.when(i == j)
            def _(j=j):
                before(j)

        @pl.when(i < 16)
        def _():
            w, h = i // 2, i % 2
            rows = pl.ds(pl.multiple_of(h * HALF, HALF), HALF)

            @pl.when(i >= 2)
            def _():
                partial_copy(h).wait_send()

            up(2 * w + 1, rows)

            def store(cs, total):
                dd_out[h, :, cs] = total

            down(2 * w + 1, h, store)

            @pl.when(i >= 2)
            def _():
                pl.semaphore_wait(dd_free.at[h], 1)

            partial_copy(h).start()

        @pl.when(i > 0)
        def _():
            w, h = (i - 1) // 2, (i - 1) % 2
            rows = pl.ds(pl.multiple_of(h * HALF, HALF), HALF)
            up(2 * w, rows)
            partial_copy(h).wait_recv()

            def store(cs, total):
                acc[w, rows, cs] = total + dd_in[h, :, cs]

            down(2 * w, h, store)

            @pl.when(i < 15)
            def _():
                pl.semaphore_signal(dd_free.at[h], inc=1, device_id=peer(1), device_id_type=MESH)

        for j in (7, 10):
            @pl.when(i == j)
            def _(j=j):
                after(j)

    reduce_start(1, PARTS[3:])
    reduce_start(2)
    reduce_start(3)

    def sum_rows(first, n, fn):
        @pl.loop(0, n // 16)
        def _(i):
            fn(pl.ds(pl.multiple_of(first + i * 16, 16), 16))

    def add(k):
        reduce_wait(k)
        for first, n, part in ((0, 480, PARTS[0]), (480, 16, PARTS[3]), (496, 16, PARTS[4])):
            w = reduce_move(part, k)[1]

            def one(rows, w=w):
                got = acc[w, rows, :] + rs[k, rows, :]
                if k == 5:
                    got = got + x_all[0, rows, :].astype(jnp.float32)
                acc[w, rows, :] = got

            sum_rows(first, n, one)

    add(0)
    add(1)
    add(2)
    reduce_start(4)
    reduce_start(5)
    add(3)
    add(4)
    core = lax.axis_index('ex') % 2

    @pl.when(core == 0)
    def _():
        reduce_last_start()

    add(5)

    @pl.when(core == 1)
    def _():
        reduce_last_start()


    drain(tiles.at[pl.ds(0, 2)], gt_send)
    drain(x_all.at[pl.ds(0, 7)], ag_send)
    drain(x_all.at[pl.ds(0, 8)], xd_send)
    for h in range(2):
        partial_copy(h).wait_send()

    def one(rows):
        y_out[rows, :] = (acc[0, rows, :] + rs[6, rows, :]).astype(y_out.dtype)

    reduce_wait(6)
    for r, n, _ in FIRST:
        sum_rows(r, n, one)
    drain(acc.at[pl.ds(0, 7)], rs_send)
    reduce_wait(7)
    for r, n, _ in SECOND:
        sum_rows(r, n, one)


def solution(mesh):
    n_dev = mesh.shape['ez'] * mesh.shape['ey'] * mesh.shape['ex']

    def local_layer(x_loc, ids_loc, gates_loc, w_g, w_u, w_d):
        tok, hid = x_loc.shape
        top_k = ids_loc.shape[1]
        n_local, _, ffn = w_g.shape
        hbm = pl.BlockSpec(memory_space=pl.ANY)
        dma = pltpu.SemaphoreType.DMA
        f32, bf16 = jnp.float32, jnp.bfloat16
        y = pl.pallas_call(
            moe_kernel,
            out_shape=pltpu.VMEM((tok, hid), bf16),
            in_specs=[hbm] * 6,
            out_specs=pl.BlockSpec(memory_space=pltpu.VMEM),
            scratch_shapes=[
                pltpu.VMEM((n_local, hid, ffn), bf16),
                pltpu.VMEM((n_local, hid, ffn), bf16),
                pltpu.VMEM((n_local, ffn, hid), bf16),
                pltpu.VMEM((top_k, tok), jnp.int32),
                pltpu.VMEM((top_k, tok), f32),
                pltpu.VMEM((n_dev, tok, hid), bf16),
                pltpu.VMEM((5, n_dev, 8, QUARTER), f32),
                pltpu.VMEM((n_dev, 8, QUARTER), f32),
                pltpu.VMEM((n_local, HALF, ffn), bf16),
                pltpu.VMEM((8, tok, hid), f32),
                pltpu.VMEM((7, tok, hid), f32),
                pltpu.VMEM((2, HALF, hid), f32),
                pltpu.VMEM((2, HALF, hid), f32),
                dma((6,)), dma, dma((5,)), dma, dma((7,)), dma, dma((8,)),
                dma, dma((8,)), dma((2,)), dma((2,)), pltpu.SemaphoreType.REGULAR((2,)),
            ],
            compiler_params=pltpu.CompilerParams(collective_id=0, has_side_effects=True, vmem_limit_bytes=62_000_000),
            name='moe_kernel',
        )(x_loc, ids_loc.T, gates_loc.T, w_g, w_u, w_d)
        return y

    tok_spec = P(TOKEN_AXES, None)
    w_spec = P(EXPERT_AXES, None, None)
    return jax.shard_map(local_layer, mesh=mesh, in_specs=(tok_spec, tok_spec, tok_spec, w_spec, w_spec, w_spec), out_specs=tok_spec, check_vma=False)
```

```python
import jax
import jax.numpy as jnp
from jax import lax
from jax.experimental import pallas as pl
from jax.experimental.pallas import tpu as pltpu
from jax.sharding import PartitionSpec as P

TOKEN_AXES = ('ez', 'ey', 'ex')
EXPERT_AXES = ('ex', 'ey', 'ez')
MESH = pl.DeviceIdType.MESH

PARTS = (
    (0, 160, (2, 4, 8), (2, 4, 8)),
    (160, 160, (4, 8, 2), (4, 8, 2)),
    (320, 160, (8, 2, 4), (8, 2, 4)),
    (480, 16, (2, 4, 8), (2, 8, 4)),
    (496, 16, (2, 4, 8), (4, 2, 8)),
)
GATHER = ((0, 0), (0, 1), (0, 2), (1, 1), (1, 2), (2, 2), (4, 2))
ONWARD = {0: (3, 4), 1: (5,), 2: (), 3: (6,), 4: (), 5: (), 6: ()}


def masks(part):
    a, b, c = part[2]
    return 0, a, b, c, a ^ b, a ^ c, b ^ c, 14


def reduce_move(part, k):
    a, b, c = part[3]
    mask, axis = ((a, a), (a ^ b, a), (14, a), (a ^ c, a), (b ^ c, b), (b, b), (c, c))[k]
    return masks(part).index(mask), masks(part).index(mask ^ axis), axis


FIRST = [(part[0], 144, part) for part in PARTS[:3]]
SECOND = [(part[0] + 144, 16, part) for part in PARTS[:3]] + [(part[0], part[1], part) for part in PARTS[3:]]
SECOND_ROWS = 80
BITS = (2, 4, 8, 1)
PATHS = {m: [b for b in BITS if m & b] for m in range(16)}
TILE_MOVES = (
    [(0, m) for m in range(1, 16)],
    [(1, m) for m in range(16) if len(PATHS[m]) > 1],
    [(2, m) for m in (7, 11, 13)],
    [(2, m) for m in (14, 15)],
    [(3, 15)],
)
HALF = 256
QUARTER = 128


def peer(mask):
    z, y, e = lax.axis_index('ez'), lax.axis_index('ey'), lax.axis_index('ex')
    x, c = e // 2, e % 2
    z = 1 - z if mask & 8 else z
    y = 1 - y if mask & 4 else y
    x = 1 - x if mask & 2 else x
    c = 1 - c if mask & 1 else c
    return z, y, 2 * x + c


def moe_kernel(x_hbm, ids_hbm, gates_hbm, w1_hbm, w3_hbm, w2_hbm, y_out,
               w1, w3, w2, ids, gates, x_all, tiles, merged, act, acc, rs, dd_out, dd_in,
               load_sem, gt_send, gt_recv, ag_send, ag_recv, xd_send, xd_recv,
               rs_send, rs_recv, dd_send, dd_recv, dd_free):
    tok = x_hbm.shape[0]

    def remote(src, dst, ssem, rsem, mask):
        return pltpu.make_async_remote_copy(src, dst, ssem, rsem, device_id=peer(mask), device_id_type=MESH)

    def drain(ref, sem):
        pltpu.make_async_copy(ref, ref, sem).wait()

    def gather_start(k):
        w, a = GATHER[k]
        for part in PARTS:
            rows = pl.ds(part[0], part[1])
            remote(x_all.at[2 * w, rows], x_all.at[2 * (k + 1), rows], ag_send, ag_recv.at[k], part[2][a]).start()

    def gather_wait(k):
        drain(x_all.at[2 * (k + 1)], ag_recv.at[k])

    def pair_copy(w):
        return remote(x_all.at[2 * w], x_all.at[2 * w + 1], xd_send, xd_recv.at[w % 2], 1)

    def reduce_start(k, parts=PARTS):
        for part in parts:
            w, _, axis = reduce_move(part, k)
            rows = pl.ds(part[0], part[1])
            remote(acc.at[w, rows], rs.at[k, rows], rs_send, rs_recv.at[k], axis).start()

    def reduce_last_start():
        for i, piece in enumerate((FIRST, SECOND)):
            for r, n, part in piece:
                w, _, axis = reduce_move(part, 6)
                rows = pl.ds(r, n)
                remote(acc.at[w, rows], rs.at[6, rows], rs_send, rs_recv.at[6 + i], axis).start()

    def reduce_wait(k):
        rows = tok if k < 6 else SECOND_ROWS if k == 7 else tok - SECOND_ROWS
        drain(acc.at[0, pl.ds(0, rows)], rs_recv.at[k])

    def partial_copy(s):
        return remote(dd_out.at[s], dd_in.at[s], dd_send.at[s], dd_recv.at[s], 1)

    def tiles_start(g):
        for hop, m in TILE_MOVES[g]:
            remote(tiles.at[hop, m], tiles.at[hop + 1, m], gt_send, gt_recv.at[g], PATHS[m][hop]).start()

    def tiles_wait(g):
        drain(tiles.at[0, pl.ds(0, len(TILE_MOVES[g]))], gt_recv.at[g])

    x_load = pltpu.make_async_copy(x_hbm, x_all.at[0], load_sem.at[0])
    loads = [pltpu.make_async_copy(s, d, load_sem.at[i]) for i, s, d in (
        (1, ids_hbm, ids), (1, gates_hbm, gates), (2, w1_hbm, w1), (2, w3_hbm, w3), (2, w2_hbm, w2))]

    barrier = pltpu.get_barrier_semaphore()
    for mask in BITS:
        pl.semaphore_signal(barrier, inc=1, device_id=peer(mask), device_id_type=MESH)
    x_load.start()
    for c in loads:
        c.start()
    drain(tiles.at[0, pl.ds(0, 8)], load_sem.at[1])
    for m in range(16):
        z, y, e = peer(m)
        for l in range(2):
            hit = ids[...] == 2 * (e * 4 + y * 2 + z) + l
            row = jnp.sum(jnp.where(hit, gates[...], 0.0), axis=0, keepdims=True)
            for q in range(4):
                tiles[0, m, pl.ds(2 * q + l, 1), :] = row[:, q * QUARTER:(q + 1) * QUARTER]
    x_load.wait()
    pl.semaphore_wait(barrier, 4)
    tiles_start(0)
    gather_start(0)
    pair_copy(0).start()
    tiles_wait(0)
    tiles_start(1)
    gather_start(1)
    gather_start(2)
    drain(x_all.at[pl.ds(0, 6)], load_sem.at[2])

    def merge_tiles(w):
        token = lax.broadcasted_iota(jnp.int32, (8, QUARTER), 0) // 2 * QUARTER + lax.broadcasted_iota(jnp.int32, (8, QUARTER), 1)
        for side in range(2):
            tile = None
            for part in PARTS:
                m = masks(part)[w] | side
                mine = tiles[len(PATHS[m]), m]
                tile = mine if tile is None else jnp.where(token < part[0], tile, mine)
            merged[2 * w + side] = tile

    def before(j):
        if j % 2 == 1 and j < 14:
            w = (j + 1) // 2
            gather_wait(w - 1)
            for k in ONWARD[w - 1]:
                gather_start(k)
            pair_copy(w).start()
        if j == 1:
            tiles_wait(1)
            tiles_start(2)
            tiles_start(3)
        if j == 8:
            tiles_wait(2)
        if j == 13:
            tiles_wait(3)
            tiles_start(4)
        if j == 14:
            tiles_wait(4)
        if j % 2 == 0 and j < 16:
            merge_tiles(j // 2)
            pair_copy(j // 2).wait_recv()

    def after(j):
        if j == 7:
            reduce_start(0)
        if j == 10:
            reduce_start(1, PARTS[:3])

    def up(slot, rows):
        for l in range(2):
            for n in range(2):
                cs = slice(n * 256, n * 256 + 256)
                x_in = x_all[slot, rows, :]
                h1 = jnp.dot(x_in, w1[l, :, cs], preferred_element_type=jnp.float32)
                h3 = jnp.dot(x_in, w3[l, :, cs], preferred_element_type=jnp.float32)
                act[l, :, cs] = (h1 * jax.nn.sigmoid(h1) * h3).astype(jnp.bfloat16)

    def down(slot, h, store):
        columns = merged[slot].T
        gate = []
        for l in range(2):
            halves = [jnp.where(h == 0, columns[:, 2 * i + l:2 * i + l + 1], columns[:, 4 + 2 * i + l:5 + 2 * i + l]) for i in range(2)]
            gate.append(jnp.concatenate(halves, axis=0))
        for n in range(4):
            cs = slice(n * 256, n * 256 + 256)
            total = None
            for l in range(2):
                o = jnp.dot(act[l], w2[l, :, cs], preferred_element_type=jnp.float32)
                o = o.astype(jnp.bfloat16).astype(jnp.float32)
                term = jnp.where(gate[l] > 0, gate[l] * o, 0.0)
                total = term if total is None else total + term
            store(cs, total)

    @pl.loop(0, 17)
    def _(i):
        for j in range(16):
            @pl.when(i == j)
            def _(j=j):
                before(j)

        @pl.when(i < 16)
        def _():
            w, h = i // 2, i % 2
            rows = pl.ds(pl.multiple_of(h * HALF, HALF), HALF)

            @pl.when(i >= 2)
            def _():
                partial_copy(h).wait_send()

            up(2 * w + 1, rows)

            def store(cs, total):
                dd_out[h, :, cs] = total

            down(2 * w + 1, h, store)

            @pl.when(i >= 2)
            def _():
                pl.semaphore_wait(dd_free.at[h], 1)

            partial_copy(h).start()

        @pl.when(i > 0)
        def _():
            w, h = (i - 1) // 2, (i - 1) % 2
            rows = pl.ds(pl.multiple_of(h * HALF, HALF), HALF)
            up(2 * w, rows)
            partial_copy(h).wait_recv()

            def store(cs, total):
                acc[w, rows, cs] = total + dd_in[h, :, cs]

            down(2 * w, h, store)

            @pl.when(i < 15)
            def _():
                pl.semaphore_signal(dd_free.at[h], inc=1, device_id=peer(1), device_id_type=MESH)

        for j in (7, 10):
            @pl.when(i == j)
            def _(j=j):
                after(j)

    reduce_start(1, PARTS[3:])
    reduce_start(2)
    reduce_start(3)

    def sum_rows(first, n, fn):
        @pl.loop(0, n // 16)
        def _(i):
            fn(pl.ds(pl.multiple_of(first + i * 16, 16), 16))

    def add(k):
        reduce_wait(k)
        for first, n, part in ((0, 480, PARTS[0]), (480, 16, PARTS[3]), (496, 16, PARTS[4])):
            w = reduce_move(part, k)[1]

            def one(rows, w=w):
                got = acc[w, rows, :] + rs[k, rows, :]
                if k == 5:
                    got = got + x_all[0, rows, :].astype(jnp.float32)
                acc[w, rows, :] = got

            sum_rows(first, n, one)

    add(0)
    add(1)
    add(2)
    reduce_start(4)
    reduce_start(5)
    add(3)
    add(4)
    core = lax.axis_index('ex') % 2

    @pl.when(core == 0)
    def _():
        reduce_last_start()

    add(5)

    @pl.when(core == 1)
    def _():
        reduce_last_start()


    drain(tiles.at[pl.ds(0, 2)], gt_send)
    drain(x_all.at[pl.ds(0, 7)], ag_send)
    drain(x_all.at[pl.ds(0, 8)], xd_send)
    for h in range(2):
        partial_copy(h).wait_send()

    def one(rows):
        y_out[rows, :] = (acc[0, rows, :] + rs[6, rows, :]).astype(y_out.dtype)

    reduce_wait(6)
    for r, n, _ in FIRST:
        sum_rows(r, n, one)
    drain(acc.at[pl.ds(0, 7)], rs_send)
    reduce_wait(7)
    for r, n, _ in SECOND:
        one(pl.ds(r, n))


def solution(mesh):
    n_dev = mesh.shape['ez'] * mesh.shape['ey'] * mesh.shape['ex']

    def local_layer(x_loc, ids_loc, gates_loc, w_g, w_u, w_d):
        tok, hid = x_loc.shape
        top_k = ids_loc.shape[1]
        n_local, _, ffn = w_g.shape
        hbm = pl.BlockSpec(memory_space=pl.ANY)
        dma = pltpu.SemaphoreType.DMA
        f32, bf16 = jnp.float32, jnp.bfloat16
        y = pl.pallas_call(
            moe_kernel,
            out_shape=pltpu.VMEM((tok, hid), bf16),
            in_specs=[hbm] * 6,
            out_specs=pl.BlockSpec(memory_space=pltpu.VMEM),
            scratch_shapes=[
                pltpu.VMEM((n_local, hid, ffn), bf16),
                pltpu.VMEM((n_local, hid, ffn), bf16),
                pltpu.VMEM((n_local, ffn, hid), bf16),
                pltpu.VMEM((top_k, tok), jnp.int32),
                pltpu.VMEM((top_k, tok), f32),
                pltpu.VMEM((n_dev, tok, hid), bf16),
                pltpu.VMEM((5, n_dev, 8, QUARTER), f32),
                pltpu.VMEM((n_dev, 8, QUARTER), f32),
                pltpu.VMEM((n_local, HALF, ffn), bf16),
                pltpu.VMEM((8, tok, hid), f32),
                pltpu.VMEM((7, tok, hid), f32),
                pltpu.VMEM((2, HALF, hid), f32),
                pltpu.VMEM((2, HALF, hid), f32),
                dma((3,)), dma, dma((5,)), dma, dma((7,)), dma, dma((2,)),
                dma, dma((8,)), dma((2,)), dma((2,)), pltpu.SemaphoreType.REGULAR((2,)),
            ],
            compiler_params=pltpu.CompilerParams(collective_id=0, has_side_effects=True, vmem_limit_bytes=62_000_000),
            name='moe_kernel',
        )(x_loc, ids_loc.T, gates_loc.T, w_g, w_u, w_d)
        return y

    tok_spec = P(TOKEN_AXES, None)
    w_spec = P(EXPERT_AXES, None, None)
    return jax.shard_map(local_layer, mesh=mesh, in_specs=(tok_spec, tok_spec, tok_spec, w_spec, w_spec, w_spec), out_specs=tok_spec, check_vma=False)
```

```python
import jax
import jax.numpy as jnp
from jax import lax
from jax.experimental import pallas as pl
from jax.experimental.pallas import tpu as pltpu
from jax.sharding import PartitionSpec as P

TOKEN_AXES = ('ez', 'ey', 'ex')
EXPERT_AXES = ('ex', 'ey', 'ez')
MESH = pl.DeviceIdType.MESH

PARTS = (
    (0, 160, (2, 4, 8), (2, 4, 8)),
    (160, 160, (4, 8, 2), (4, 8, 2)),
    (320, 160, (8, 2, 4), (8, 2, 4)),
    (480, 16, (2, 4, 8), (2, 8, 4)),
    (496, 16, (2, 4, 8), (4, 2, 8)),
)
GATHER = ((0, 0), (0, 1), (0, 2), (1, 1), (1, 2), (2, 2), (4, 2))
ONWARD = {0: (3, 4), 1: (5,), 2: (), 3: (6,), 4: (), 5: (), 6: ()}


def masks(part):
    a, b, c = part[2]
    return 0, a, b, c, a ^ b, a ^ c, b ^ c, 14


def reduce_move(part, k):
    a, b, c = part[3]
    mask, axis = ((a, a), (a ^ b, a), (14, a), (a ^ c, a), (b ^ c, b), (b, b), (c, c))[k]
    return masks(part).index(mask), masks(part).index(mask ^ axis), axis


FIRST = [(part[0], 144, part) for part in PARTS[:3]]
SECOND = [(part[0] + 144, 16, part) for part in PARTS[:3]] + [(part[0], part[1], part) for part in PARTS[3:]]
SECOND_ROWS = 80
BITS = (2, 4, 8, 1)
PATHS = {m: [b for b in BITS if m & b] for m in range(16)}
TILE_MOVES = (
    [(0, 1)],
    [(0, m) for m in range(2, 16)],
    [(1, m) for m in (3, 5, 9)],
    [(1, m) for m in (6, 7, 10, 11, 12, 13, 14, 15)],
    [(2, m) for m in (7, 11, 13)],
    [(2, m) for m in (14, 15)],
    [(3, 15)],
)
HALF = 256
QUARTER = 128


def peer(mask):
    z, y, e = lax.axis_index('ez'), lax.axis_index('ey'), lax.axis_index('ex')
    x, c = e // 2, e % 2
    z = 1 - z if mask & 8 else z
    y = 1 - y if mask & 4 else y
    x = 1 - x if mask & 2 else x
    c = 1 - c if mask & 1 else c
    return z, y, 2 * x + c


def moe_kernel(x_hbm, ids_hbm, gates_hbm, w1_hbm, w3_hbm, w2_hbm, y_out,
               w1, w3, w2, ids, gates, x_all, tiles, merged, act, acc, rs, dd_out, dd_in,
               load_sem, gt_send, gt_recv, ag_send, ag_recv, xd_send, xd_recv,
               rs_send, rs_recv, dd_send, dd_recv, dd_free, ready):
    tok = x_hbm.shape[0]

    def remote(src, dst, ssem, rsem, mask):
        return pltpu.make_async_remote_copy(src, dst, ssem, rsem, device_id=peer(mask), device_id_type=MESH)

    def drain(ref, sem):
        pltpu.make_async_copy(ref, ref, sem).wait()

    def gather_start(k):
        w, a = GATHER[k]
        for part in PARTS:
            rows = pl.ds(part[0], part[1])
            remote(x_all.at[2 * w, rows], x_all.at[2 * (k + 1), rows], ag_send, ag_recv.at[k], part[2][a]).start()

    def gather_wait(k):
        drain(x_all.at[2 * (k + 1)], ag_recv.at[k])

    def pair_copy(w):
        return remote(x_all.at[2 * w], x_all.at[2 * w + 1], xd_send, xd_recv.at[w % 2], 1)

    def reduce_start(k, parts=PARTS):
        for part in parts:
            w, _, axis = reduce_move(part, k)
            rows = pl.ds(part[0], part[1])
            remote(acc.at[w, rows], rs.at[k, rows], rs_send, rs_recv.at[k], axis).start()

    def reduce_last_start():
        for i, piece in enumerate((FIRST, SECOND)):
            for r, n, part in piece:
                w, _, axis = reduce_move(part, 6)
                rows = pl.ds(r, n)
                remote(acc.at[w, rows], rs.at[6, rows], rs_send, rs_recv.at[6 + i], axis).start()

    def reduce_wait(k):
        rows = tok if k < 6 else SECOND_ROWS if k == 7 else tok - SECOND_ROWS
        drain(acc.at[0, pl.ds(0, rows)], rs_recv.at[k])

    def partial_copy(s):
        return remote(dd_out.at[s], dd_in.at[s], dd_send.at[s], dd_recv.at[s], 1)

    def tiles_start(g):
        for hop, m in TILE_MOVES[g]:
            remote(tiles.at[hop, m], tiles.at[hop + 1, m], gt_send, gt_recv.at[g], PATHS[m][hop]).start()

    def tiles_wait(g):
        drain(tiles.at[0, pl.ds(0, len(TILE_MOVES[g]))], gt_recv.at[g])

    loads = [pltpu.make_async_copy(s, d, load_sem.at[i]) for i, s, d in (
        (0, x_hbm, x_all.at[0]), (1, ids_hbm, ids), (1, gates_hbm, gates), (2, w1_hbm, w1), (2, w3_hbm, w3), (2, w2_hbm, w2))]

    z, y, e = lax.axis_index('ez'), lax.axis_index('ey'), lax.axis_index('ex')
    answers = {8: z, 4: y, 2: e // 2, 1: 1 - e % 2}
    barrier = pltpu.get_barrier_semaphore()
    for bit in BITS:
        @pl.when(answers[bit] == 0)
        def _(bit=bit):
            pl.semaphore_signal(barrier, inc=1, device_id=peer(bit), device_id_type=MESH)
    for c in loads:
        c.start()
    expected = z + y + e // 2 + 1 - e % 2

    @pl.when(expected > 0)
    def _():
        pl.semaphore_wait(barrier, expected)

    for i, bit in enumerate(BITS):
        @pl.when(answers[bit] == 1)
        def _(i=i, bit=bit):
            pl.semaphore_signal(ready.at[i], inc=1, device_id=peer(bit), device_id_type=MESH)

    def first_rows(bit):
        for part in PARTS:
            if part[2][0] == bit:
                rows = pl.ds(part[0], part[1])
                remote(x_hbm.at[rows], x_all.at[2, rows], ag_send, ag_recv.at[0], bit).start()
        if bit == 1:
            pair_copy(0).start()

    for bit in BITS[:3]:
        @pl.when(answers[bit] == 1)
        def _(bit=bit):
            first_rows(bit)
    loads[0].wait()

    @pl.when(answers[1] == 1)
    def _():
        first_rows(1)

    drain(tiles.at[0, pl.ds(0, 8)], load_sem.at[1])
    for m in range(16):
        z, y, e = peer(m)
        for l in range(2):
            hit = ids[...] == 2 * (e * 4 + y * 2 + z) + l
            row = jnp.sum(jnp.where(hit, gates[...], 0.0), axis=0, keepdims=True)
            for q in range(4):
                tiles[0, m, pl.ds(2 * q + l, 1), :] = row[:, q * QUARTER:(q + 1) * QUARTER]
    for i, bit in enumerate(BITS):
        @pl.when(answers[bit] == 0)
        def _(i=i, bit=bit):
            pl.semaphore_wait(ready.at[i], 1)
            first_rows(bit)
    tiles_start(0)
    tiles_start(1)
    gather_start(1)
    gather_start(2)
    drain(x_all.at[pl.ds(0, 6)], load_sem.at[2])
    tiles_wait(0)

    def merge_tiles(w):
        token = lax.broadcasted_iota(jnp.int32, (8, QUARTER), 0) // 2 * QUARTER + lax.broadcasted_iota(jnp.int32, (8, QUARTER), 1)
        for side in range(2):
            tile = None
            for part in PARTS:
                m = masks(part)[w] | side
                mine = tiles[len(PATHS[m]), m]
                tile = mine if tile is None else jnp.where(token < part[0], tile, mine)
            merged[2 * w + side] = tile

    def before(j):
        for g, onward in {1: ((1, (2, 3)),), 2: ((2, ()),), 7: ((3, (4, 5)),), 8: ((4, ()),), 13: ((5, (6,)),), 14: ((6, ()),)}.get(j, ()):
            tiles_wait(g)
            for k in onward:
                tiles_start(k)
        if j % 2 == 1 and j < 14:
            w = (j + 1) // 2
            gather_wait(w - 1)
            for k in ONWARD[w - 1]:
                gather_start(k)
            pair_copy(w).start()
        if j % 2 == 0 and j < 16:
            merge_tiles(j // 2)
            pair_copy(j // 2).wait_recv()

    def after(j):
        if j == 7:
            reduce_start(0)
        if j == 10:
            reduce_start(1, PARTS[:3])

    def up(slot, rows):
        for l in range(2):
            for n in range(2):
                cs = slice(n * 256, n * 256 + 256)
                x_in = x_all[slot, rows, :]
                h1 = jnp.dot(x_in, w1[l, :, cs], preferred_element_type=jnp.float32)
                h3 = jnp.dot(x_in, w3[l, :, cs], preferred_element_type=jnp.float32)
                act[l, :, cs] = (h1 * jax.nn.sigmoid(h1) * h3).astype(jnp.bfloat16)

    def down(slot, h, store):
        columns = merged[slot].T
        gate = []
        for l in range(2):
            halves = [jnp.where(h == 0, columns[:, 2 * i + l:2 * i + l + 1], columns[:, 4 + 2 * i + l:5 + 2 * i + l]) for i in range(2)]
            gate.append(jnp.concatenate(halves, axis=0))
        for n in range(4):
            cs = slice(n * 256, n * 256 + 256)
            total = None
            for l in range(2):
                o = jnp.dot(act[l], w2[l, :, cs], preferred_element_type=jnp.float32)
                o = o.astype(jnp.bfloat16).astype(jnp.float32)
                term = jnp.where(gate[l] > 0, gate[l] * o, 0.0)
                total = term if total is None else total + term
            store(cs, total)

    @pl.loop(0, 17)
    def _(i):
        for j in range(16):
            @pl.when(i == j)
            def _(j=j):
                before(j)

        @pl.when(i < 16)
        def _():
            w, h = i // 2, i % 2
            rows = pl.ds(pl.multiple_of(h * HALF, HALF), HALF)

            @pl.when(i >= 2)
            def _():
                partial_copy(h).wait_send()

            up(2 * w + 1, rows)

            def store(cs, total):
                dd_out[h, :, cs] = total

            down(2 * w + 1, h, store)

            @pl.when(i >= 2)
            def _():
                pl.semaphore_wait(dd_free.at[h], 1)

            partial_copy(h).start()

        @pl.when(i > 0)
        def _():
            w, h = (i - 1) // 2, (i - 1) % 2
            rows = pl.ds(pl.multiple_of(h * HALF, HALF), HALF)
            up(2 * w, rows)
            partial_copy(h).wait_recv()

            def store(cs, total):
                acc[w, rows, cs] = total + dd_in[h, :, cs]

            down(2 * w, h, store)

            @pl.when(i < 15)
            def _():
                pl.semaphore_signal(dd_free.at[h], inc=1, device_id=peer(1), device_id_type=MESH)

        for j in (7, 10):
            @pl.when(i == j)
            def _(j=j):
                after(j)

    reduce_start(1, PARTS[3:])
    reduce_start(2)
    reduce_start(3)

    def sum_rows(first, n, fn):
        @pl.loop(0, n // 16)
        def _(i):
            fn(pl.ds(pl.multiple_of(first + i * 16, 16), 16))

    def add(k):
        reduce_wait(k)
        for first, n, part in ((0, 480, PARTS[0]), (480, 16, PARTS[3]), (496, 16, PARTS[4])):
            w = reduce_move(part, k)[1]

            def one(rows, w=w):
                got = acc[w, rows, :] + rs[k, rows, :]
                if k == 5:
                    got = got + x_all[0, rows, :].astype(jnp.float32)
                acc[w, rows, :] = got

            sum_rows(first, n, one)

    add(0)
    add(1)
    add(2)
    reduce_start(4)
    reduce_start(5)
    add(3)
    add(4)
    core = lax.axis_index('ex') % 2

    @pl.when(core == 0)
    def _():
        reduce_last_start()

    add(5)

    @pl.when(core == 1)
    def _():
        reduce_last_start()


    drain(tiles.at[pl.ds(0, 2)], gt_send)
    drain(x_all.at[pl.ds(0, 7)], ag_send)
    drain(x_all.at[pl.ds(0, 8)], xd_send)
    for h in range(2):
        partial_copy(h).wait_send()

    def one(rows):
        y_out[rows, :] = (acc[0, rows, :] + rs[6, rows, :]).astype(y_out.dtype)

    reduce_wait(6)
    for r, n, _ in FIRST:
        sum_rows(r, n, one)
    drain(acc.at[pl.ds(0, 7)], rs_send)
    reduce_wait(7)
    for r, n, _ in SECOND:
        one(pl.ds(r, n))


def solution(mesh):
    n_dev = mesh.shape['ez'] * mesh.shape['ey'] * mesh.shape['ex']

    def local_layer(x_loc, ids_loc, gates_loc, w_g, w_u, w_d):
        tok, hid = x_loc.shape
        top_k = ids_loc.shape[1]
        n_local, _, ffn = w_g.shape
        hbm = pl.BlockSpec(memory_space=pl.ANY)
        dma = pltpu.SemaphoreType.DMA
        f32, bf16 = jnp.float32, jnp.bfloat16
        y = pl.pallas_call(
            moe_kernel,
            out_shape=pltpu.VMEM((tok, hid), bf16),
            in_specs=[hbm] * 6,
            out_specs=pl.BlockSpec(memory_space=pltpu.VMEM),
            scratch_shapes=[
                pltpu.VMEM((n_local, hid, ffn), bf16),
                pltpu.VMEM((n_local, hid, ffn), bf16),
                pltpu.VMEM((n_local, ffn, hid), bf16),
                pltpu.VMEM((top_k, tok), jnp.int32),
                pltpu.VMEM((top_k, tok), f32),
                pltpu.VMEM((n_dev, tok, hid), bf16),
                pltpu.VMEM((5, n_dev, 8, QUARTER), f32),
                pltpu.VMEM((n_dev, 8, QUARTER), f32),
                pltpu.VMEM((n_local, HALF, ffn), bf16),
                pltpu.VMEM((8, tok, hid), f32),
                pltpu.VMEM((7, tok, hid), f32),
                pltpu.VMEM((2, HALF, hid), f32),
                pltpu.VMEM((2, HALF, hid), f32),
                dma((3,)), dma, dma((7,)), dma, dma((7,)), dma, dma((2,)),
                dma, dma((8,)), dma((2,)), dma((2,)), pltpu.SemaphoreType.REGULAR((2,)), pltpu.SemaphoreType.REGULAR((4,)),
            ],
            compiler_params=pltpu.CompilerParams(collective_id=0, has_side_effects=True, vmem_limit_bytes=62_000_000),
            name='moe_kernel',
        )(x_loc, ids_loc.T, gates_loc.T, w_g, w_u, w_d)
        return y

    tok_spec = P(TOKEN_AXES, None)
    w_spec = P(EXPERT_AXES, None, None)
    return jax.shard_map(local_layer, mesh=mesh, in_specs=(tok_spec, tok_spec, tok_spec, w_spec, w_spec, w_spec), out_specs=tok_spec, check_vma=False)
```

```python
import jax
import jax.numpy as jnp
from jax import lax
from jax.experimental import pallas as pl
from jax.experimental.pallas import tpu as pltpu
from jax.sharding import PartitionSpec as P

TOKEN_AXES = ('ez', 'ey', 'ex')
EXPERT_AXES = ('ex', 'ey', 'ez')
MESH = pl.DeviceIdType.MESH

PARTS = (
    (0, 160, (2, 4, 8), (2, 4, 8)),
    (160, 160, (4, 8, 2), (4, 8, 2)),
    (320, 160, (8, 2, 4), (8, 2, 4)),
    (480, 16, (2, 4, 8), (2, 8, 4)),
    (496, 16, (2, 4, 8), (4, 2, 8)),
)
GATHER = ((0, 0), (0, 1), (0, 2), (1, 1), (1, 2), (2, 2), (4, 2))
ONWARD = {0: (3, 4), 1: (5,), 2: (), 3: (6,), 4: (), 5: (), 6: ()}


def masks(part):
    a, b, c = part[2]
    return 0, a, b, c, a ^ b, a ^ c, b ^ c, 14


def reduce_move(part, k):
    a, b, c = part[3]
    mask, axis = ((a, a), (a ^ b, a), (14, a), (a ^ c, a), (b ^ c, b), (b, b), (c, c))[k]
    return masks(part).index(mask), masks(part).index(mask ^ axis), axis


FIRST = [(part[0], 144, part) for part in PARTS[:3]] + [(part[0], part[1], part) for part in PARTS[3:]]
SECOND = [(part[0] + 144, 16, part) for part in PARTS[:3]]
SECOND_ROWS = 48
BITS = (2, 4, 8, 1)
PATHS = {m: [b for b in BITS if m & b] for m in range(16)}
TILE_MOVES = (
    [(0, 1)],
    [(0, m) for m in range(2, 16)],
    [(1, m) for m in (3, 5, 9)],
    [(1, m) for m in (6, 7, 10, 11, 12, 13, 14, 15)],
    [(2, m) for m in (7, 11, 13)],
    [(2, m) for m in (14, 15)],
    [(3, 15)],
)
HALF = 256
QUARTER = 128


def peer(mask):
    z, y, e = lax.axis_index('ez'), lax.axis_index('ey'), lax.axis_index('ex')
    x, c = e // 2, e % 2
    z = 1 - z if mask & 8 else z
    y = 1 - y if mask & 4 else y
    x = 1 - x if mask & 2 else x
    c = 1 - c if mask & 1 else c
    return z, y, 2 * x + c


def moe_kernel(x_hbm, ids_hbm, gates_hbm, w1_hbm, w3_hbm, w2_hbm, y_out,
               w1, w3, w2, ids, gates, x_all, tiles, merged, act, acc, rs, dd_out, dd_in,
               load_sem, gt_send, gt_recv, ag_send, ag_recv, xd_recv,
               rs_send, rs_recv, dd_send, dd_recv, dd_free, ready):
    tok = x_hbm.shape[0]

    def remote(src, dst, ssem, rsem, mask):
        return pltpu.make_async_remote_copy(src, dst, ssem, rsem, device_id=peer(mask), device_id_type=MESH)

    def drain(ref, sem):
        pltpu.make_async_copy(ref, ref, sem).wait()

    def gather_start(k):
        w, a = GATHER[k]
        for part in PARTS:
            rows = pl.ds(part[0], part[1])
            remote(x_all.at[2 * w, rows], x_all.at[2 * (k + 1), rows], ag_send, ag_recv.at[k], part[2][a]).start()

    def gather_wait(k):
        drain(x_all.at[2 * (k + 1)], ag_recv.at[k])

    def pair_copy(w):
        return remote(x_all.at[2 * w], x_all.at[2 * w + 1], ag_send, xd_recv.at[w % 2], 1)

    def sum_sem(k):
        return rs_recv.at[k] if k < 2 else ag_recv.at[k - 2] if k < 6 else gt_recv.at[k - 5]

    def reduce_start(k, parts=PARTS):
        for part in parts:
            w, _, axis = reduce_move(part, k)
            rows = pl.ds(part[0], part[1])
            remote(acc.at[w, rows], rs.at[k, rows], rs_send, sum_sem(k), axis).start()

    def reduce_last_start():
        for i, piece in enumerate((FIRST, SECOND)):
            for r, n, part in piece:
                w, _, axis = reduce_move(part, 6)
                rows = pl.ds(r, n)
                remote(acc.at[w, rows], rs.at[6, rows], rs_send, sum_sem(6 + i), axis).start()

    def reduce_wait(k):
        rows = tok if k < 6 else SECOND_ROWS if k == 7 else tok - SECOND_ROWS
        drain(acc.at[0, pl.ds(0, rows)], sum_sem(k))

    def partial_copy(s):
        return remote(dd_out.at[s], dd_in.at[s], dd_send.at[s], dd_recv.at[s], 1)

    def tiles_start(g):
        for hop, m in TILE_MOVES[g]:
            remote(tiles.at[hop, m], tiles.at[hop + 1, m], gt_send, gt_recv.at[g], PATHS[m][hop]).start()

    def tiles_wait(g):
        drain(tiles.at[0, pl.ds(0, len(TILE_MOVES[g]))], gt_recv.at[g])

    loads = [pltpu.make_async_copy(s, d, load_sem.at[i]) for i, s, d in (
        (0, x_hbm, x_all.at[0]), (1, ids_hbm, ids), (1, gates_hbm, gates), (2, w1_hbm, w1), (2, w3_hbm, w3), (2, w2_hbm, w2))]

    z, y, e = lax.axis_index('ez'), lax.axis_index('ey'), lax.axis_index('ex')
    answers = {8: z, 4: y, 2: e // 2, 1: 1 - e % 2}
    barrier = pltpu.get_barrier_semaphore()
    for bit in BITS:
        @pl.when(answers[bit] == 0)
        def _(bit=bit):
            pl.semaphore_signal(barrier, inc=1, device_id=peer(bit), device_id_type=MESH)
    for c in loads:
        c.start()
    expected = z + y + e // 2 + 1 - e % 2

    @pl.when(expected > 0)
    def _():
        pl.semaphore_wait(barrier, expected)

    for i, bit in enumerate(BITS):
        @pl.when(answers[bit] == 1)
        def _(i=i, bit=bit):
            pl.semaphore_signal(ready.at[i], inc=1, device_id=peer(bit), device_id_type=MESH)

    def first_rows(bit):
        for part in PARTS:
            if part[2][0] == bit:
                rows = pl.ds(part[0], part[1])
                remote(x_hbm.at[rows], x_all.at[2, rows], ag_send, ag_recv.at[0], bit).start()
        if bit == 1:
            pair_copy(0).start()

    for bit in BITS[:3]:
        @pl.when(answers[bit] == 1)
        def _(bit=bit):
            first_rows(bit)
    loads[0].wait()

    @pl.when(answers[1] == 1)
    def _():
        first_rows(1)

    drain(tiles.at[0, pl.ds(0, 8)], load_sem.at[1])
    for m in range(16):
        z, y, e = peer(m)
        for l in range(2):
            hit = ids[...] == 2 * (e * 4 + y * 2 + z) + l
            row = jnp.sum(jnp.where(hit, gates[...], 0.0), axis=0, keepdims=True)
            for q in range(4):
                tiles[0, m, pl.ds(2 * q + l, 1), :] = row[:, q * QUARTER:(q + 1) * QUARTER]
    for i, bit in enumerate(BITS):
        @pl.when(answers[bit] == 0)
        def _(i=i, bit=bit):
            pl.semaphore_wait(ready.at[i], 1)
            first_rows(bit)
    tiles_start(0)
    tiles_start(1)
    gather_start(1)
    gather_start(2)
    drain(x_all.at[pl.ds(0, 6)], load_sem.at[2])
    tiles_wait(0)

    def merge_tiles(w):
        token = lax.broadcasted_iota(jnp.int32, (8, QUARTER), 0) // 2 * QUARTER + lax.broadcasted_iota(jnp.int32, (8, QUARTER), 1)
        for side in range(2):
            tile = None
            for part in PARTS:
                m = masks(part)[w] | side
                mine = tiles[len(PATHS[m]), m]
                tile = mine if tile is None else jnp.where(token < part[0], tile, mine)
            merged[2 * w + side] = tile

    def before(j):
        for g, onward in {1: ((1, (2, 3)),), 2: ((2, ()),), 7: ((3, (4, 5)),), 8: ((4, ()),), 13: ((5, (6,)),), 14: ((6, ()),)}.get(j, ()):
            tiles_wait(g)
            for k in onward:
                tiles_start(k)
        if j % 2 == 1 and j < 14:
            w = (j + 1) // 2
            gather_wait(w - 1)
            for k in ONWARD[w - 1]:
                gather_start(k)
            pair_copy(w).start()
        if j % 2 == 0 and j < 16:
            merge_tiles(j // 2)
            pair_copy(j // 2).wait_recv()

    def after(j):
        if j == 7:
            reduce_start(0)
        if j == 10:
            reduce_start(1, PARTS[:3])

    def up(slot, rows):
        for l in range(2):
            for n in range(2):
                cs = slice(n * 256, n * 256 + 256)
                x_in = x_all[slot, rows, :]
                h1 = jnp.dot(x_in, w1[l, :, cs], preferred_element_type=jnp.float32)
                h3 = jnp.dot(x_in, w3[l, :, cs], preferred_element_type=jnp.float32)
                act[l, :, cs] = (h1 * jax.nn.sigmoid(h1) * h3).astype(jnp.bfloat16)

    def down(slot, h, store):
        columns = merged[slot].T
        gate = []
        for l in range(2):
            halves = [jnp.where(h == 0, columns[:, 2 * i + l:2 * i + l + 1], columns[:, 4 + 2 * i + l:5 + 2 * i + l]) for i in range(2)]
            gate.append(jnp.concatenate(halves, axis=0))
        for n in range(4):
            cs = slice(n * 256, n * 256 + 256)
            total = None
            for l in range(2):
                o = jnp.dot(act[l], w2[l, :, cs], preferred_element_type=jnp.float32)
                o = o.astype(jnp.bfloat16).astype(jnp.float32)
                term = jnp.where(gate[l] > 0, gate[l] * o, 0.0)
                total = term if total is None else total + term
            store(cs, total)

    @pl.loop(0, 17)
    def _(i):
        for j in range(16):
            @pl.when(i == j)
            def _(j=j):
                before(j)

        @pl.when(i < 16)
        def _():
            w, h = i // 2, i % 2
            rows = pl.ds(pl.multiple_of(h * HALF, HALF), HALF)

            @pl.when(i >= 2)
            def _():
                partial_copy(h).wait_send()

            up(2 * w + 1, rows)

            def store(cs, total):
                dd_out[h, :, cs] = total

            down(2 * w + 1, h, store)

            @pl.when(i >= 2)
            def _():
                pl.semaphore_wait(dd_free.at[h], 1)

            partial_copy(h).start()

        @pl.when(i > 0)
        def _():
            w, h = (i - 1) // 2, (i - 1) % 2
            rows = pl.ds(pl.multiple_of(h * HALF, HALF), HALF)
            up(2 * w, rows)
            partial_copy(h).wait_recv()

            def store(cs, total):
                acc[w, rows, cs] = total + dd_in[h, :, cs]

            down(2 * w, h, store)

            @pl.when(i < 15)
            def _():
                pl.semaphore_signal(dd_free.at[h], inc=1, device_id=peer(1), device_id_type=MESH)

        for j in (7, 10):
            @pl.when(i == j)
            def _(j=j):
                after(j)

    reduce_start(1, PARTS[3:])
    reduce_start(2)
    reduce_start(3)

    def sum_rows(first, n, fn):
        @pl.loop(0, n // 16)
        def _(i):
            fn(pl.ds(pl.multiple_of(first + i * 16, 16), 16))

    def add(k):
        reduce_wait(k)
        for first, n, part in ((0, 480, PARTS[0]), (480, 16, PARTS[3]), (496, 16, PARTS[4])):
            w = reduce_move(part, k)[1]

            def one(rows, w=w):
                got = acc[w, rows, :] + rs[k, rows, :]
                if k == 5:
                    got = got + x_all[0, rows, :].astype(jnp.float32)
                acc[w, rows, :] = got

            sum_rows(first, n, one)

    add(0)
    add(1)
    add(2)
    reduce_start(4)
    reduce_start(5)
    add(3)
    add(4)
    core = lax.axis_index('ex') % 2

    @pl.when(core == 0)
    def _():
        reduce_last_start()

    add(5)

    @pl.when(core == 1)
    def _():
        reduce_last_start()


    drain(tiles.at[pl.ds(0, 2)], gt_send)
    drain(x_all.at[pl.ds(0, 15)], ag_send)
    for h in range(2):
        partial_copy(h).wait_send()

    def one(rows):
        y_out[rows, :] = (acc[0, rows, :] + rs[6, rows, :]).astype(y_out.dtype)

    reduce_wait(6)
    for r, n, _ in FIRST:
        sum_rows(r, n, one)
    drain(acc.at[pl.ds(0, 7)], rs_send)
    reduce_wait(7)
    for r, n, _ in SECOND:
        one(pl.ds(r, n))


def solution(mesh):
    n_dev = mesh.shape['ez'] * mesh.shape['ey'] * mesh.shape['ex']

    def local_layer(x_loc, ids_loc, gates_loc, w_g, w_u, w_d):
        tok, hid = x_loc.shape
        top_k = ids_loc.shape[1]
        n_local, _, ffn = w_g.shape
        hbm = pl.BlockSpec(memory_space=pl.ANY)
        dma = pltpu.SemaphoreType.DMA
        f32, bf16 = jnp.float32, jnp.bfloat16
        y = pl.pallas_call(
            moe_kernel,
            out_shape=pltpu.VMEM((tok, hid), bf16),
            in_specs=[hbm] * 6,
            out_specs=pl.BlockSpec(memory_space=pltpu.VMEM),
            scratch_shapes=[
                pltpu.VMEM((n_local, hid, ffn), bf16),
                pltpu.VMEM((n_local, hid, ffn), bf16),
                pltpu.VMEM((n_local, ffn, hid), bf16),
                pltpu.VMEM((top_k, tok), jnp.int32),
                pltpu.VMEM((top_k, tok), f32),
                pltpu.VMEM((n_dev, tok, hid), bf16),
                pltpu.VMEM((5, n_dev, 8, QUARTER), f32),
                pltpu.VMEM((n_dev, 8, QUARTER), f32),
                pltpu.VMEM((n_local, HALF, ffn), bf16),
                pltpu.VMEM((8, tok, hid), f32),
                pltpu.VMEM((7, tok, hid), f32),
                pltpu.VMEM((2, HALF, hid), f32),
                pltpu.VMEM((2, HALF, hid), f32),
                dma((3,)), dma, dma((7,)), dma, dma((7,)), dma((2,)),
                dma, dma((2,)), dma((2,)), dma((2,)), pltpu.SemaphoreType.REGULAR((2,)), pltpu.SemaphoreType.REGULAR((4,)),
            ],
            compiler_params=pltpu.CompilerParams(collective_id=0, has_side_effects=True, vmem_limit_bytes=62_000_000),
            name='moe_kernel',
        )(x_loc, ids_loc.T, gates_loc.T, w_g, w_u, w_d)
        return y

    tok_spec = P(TOKEN_AXES, None)
    w_spec = P(EXPERT_AXES, None, None)
    return jax.shard_map(local_layer, mesh=mesh, in_specs=(tok_spec, tok_spec, tok_spec, w_spec, w_spec, w_spec), out_specs=tok_spec, check_vma=False)
```

```python
import jax
import jax.numpy as jnp
from jax import lax
from jax.experimental import pallas as pl
from jax.experimental.pallas import tpu as pltpu
from jax.sharding import PartitionSpec as P

TOKEN_AXES = ('ez', 'ey', 'ex')
EXPERT_AXES = ('ex', 'ey', 'ez')
MESH = pl.DeviceIdType.MESH

PARTS = (
    (0, 160, (2, 4, 8), (2, 4, 8)),
    (160, 160, (4, 8, 2), (4, 8, 2)),
    (320, 160, (8, 2, 4), (8, 2, 4)),
    (480, 16, (2, 4, 8), (2, 8, 4)),
    (496, 16, (2, 4, 8), (4, 2, 8)),
)
GATHER = ((0, 0), (0, 1), (0, 2), (1, 1), (1, 2), (2, 2), (4, 2))
ONWARD = {0: (3, 4), 1: (5,), 2: (), 3: (6,), 4: (), 5: (), 6: ()}


def masks(part):
    a, b, c = part[2]
    return 0, a, b, c, a ^ b, a ^ c, b ^ c, 14


def reduce_move(part, k):
    a, b, c = part[3]
    mask, axis = ((a, a), (a ^ b, a), (14, a), (a ^ c, a), (b ^ c, b), (b, b), (c, c))[k]
    return masks(part).index(mask), masks(part).index(mask ^ axis), axis


FIRST = [(part[0], 144, part) for part in PARTS[:3]] + [(part[0], part[1], part) for part in PARTS[3:]]
SECOND = [(part[0] + 144, 16, part) for part in PARTS[:3]]
SECOND_ROWS = 48
BITS = (2, 4, 8, 1)
PATHS = {m: [b for b in BITS if m & b] for m in range(16)}
TILE_MOVES = (
    [(0, 1)],
    [(0, m) for m in range(2, 16)],
    [(1, m) for m in (3, 5, 9)],
    [(1, m) for m in (6, 7, 10, 11, 12, 13, 14, 15)],
    [(2, m) for m in (7, 11, 13)],
    [(2, m) for m in (14, 15)],
    [(3, 15)],
)
HALF = 256
QUARTER = 128


def peer(mask):
    z, y, e = lax.axis_index('ez'), lax.axis_index('ey'), lax.axis_index('ex')
    x, c = e // 2, e % 2
    z = 1 - z if mask & 8 else z
    y = 1 - y if mask & 4 else y
    x = 1 - x if mask & 2 else x
    c = 1 - c if mask & 1 else c
    return z, y, 2 * x + c


def moe_kernel(x_hbm, ids_hbm, gates_hbm, w1_hbm, w3_hbm, w2_hbm, y_out,
               w1, w3, w2, ids, gates, x_all, tiles, merged, act, acc, rs, dd_out, dd_in,
               load_sem, gt_send, gt_recv, ag_send, ag_recv, xd_recv,
               rs_send, ready):
    tok = x_hbm.shape[0]

    def remote(src, dst, ssem, rsem, mask):
        return pltpu.make_async_remote_copy(src, dst, ssem, rsem, device_id=peer(mask), device_id_type=MESH)

    def drain(ref, sem):
        pltpu.make_async_copy(ref, ref, sem).wait()

    def gather_start(k):
        w, a = GATHER[k]
        for part in PARTS:
            rows = pl.ds(part[0], part[1])
            remote(x_all.at[2 * w, rows], x_all.at[2 * (k + 1), rows], ag_send, ag_recv.at[k], part[2][a]).start()

    def gather_wait(k):
        drain(x_all.at[2 * (k + 1)], ag_recv.at[k])

    def pair_copy(w):
        return remote(x_all.at[2 * w], x_all.at[2 * w + 1], ag_send, xd_recv.at[w % 2], 1)

    def sum_sem(k):
        return (gt_recv.at[0], ag_recv.at[0], ag_recv.at[1], ag_recv.at[2], ag_recv.at[3], gt_recv.at[3], gt_recv.at[1], gt_recv.at[2])[k]

    def reduce_start(k, parts=PARTS):
        for part in parts:
            w, _, axis = reduce_move(part, k)
            rows = pl.ds(part[0], part[1])
            remote(acc.at[w, rows], rs.at[k, rows], rs_send, sum_sem(k), axis).start()

    def reduce_last_start():
        for i, piece in enumerate((FIRST, SECOND)):
            for r, n, part in piece:
                w, _, axis = reduce_move(part, 6)
                rows = pl.ds(r, n)
                remote(acc.at[w, rows], rs.at[6, rows], rs_send, sum_sem(6 + i), axis).start()

    def reduce_wait(k):
        rows = tok if k < 6 else SECOND_ROWS if k == 7 else tok - SECOND_ROWS
        drain(acc.at[0, pl.ds(0, rows)], sum_sem(k))

    def partial_copy(s):
        return remote(dd_out.at[s], dd_in.at[s], load_sem.at[2 + s], load_sem.at[s], 1)

    def tiles_start(g):
        for hop, m in TILE_MOVES[g]:
            remote(tiles.at[hop, m], tiles.at[hop + 1, m], gt_send, gt_recv.at[4 if g == 6 else g], PATHS[m][hop]).start()

    def tiles_wait(g):
        drain(tiles.at[0, pl.ds(0, len(TILE_MOVES[g]))], gt_recv.at[4 if g == 6 else g])

    loads = [pltpu.make_async_copy(s, d, load_sem.at[i]) for i, s, d in (
        (0, x_hbm, x_all.at[0]), (1, ids_hbm, ids), (1, gates_hbm, gates), (2, w1_hbm, w1), (2, w3_hbm, w3), (2, w2_hbm, w2))]

    z, y, e = lax.axis_index('ez'), lax.axis_index('ey'), lax.axis_index('ex')
    answers = {8: z, 4: y, 2: e // 2, 1: 1 - e % 2}
    barrier = pltpu.get_barrier_semaphore()
    for bit in BITS:
        @pl.when(answers[bit] == 0)
        def _(bit=bit):
            pl.semaphore_signal(barrier, inc=1, device_id=peer(bit), device_id_type=MESH)
    for c in loads:
        c.start()
    expected = z + y + e // 2 + 1 - e % 2

    @pl.when(expected > 0)
    def _():
        pl.semaphore_wait(barrier, expected)

    for i, bit in enumerate(BITS):
        @pl.when(answers[bit] == 1)
        def _(i=i, bit=bit):
            pl.semaphore_signal(ready.at[i], inc=1, device_id=peer(bit), device_id_type=MESH)

    def first_rows(bit):
        for part in PARTS:
            if part[2][0] == bit:
                rows = pl.ds(part[0], part[1])
                remote(x_hbm.at[rows], x_all.at[2, rows], ag_send, ag_recv.at[0], bit).start()
        if bit == 1:
            pair_copy(0).start()

    for bit in BITS[:3]:
        @pl.when(answers[bit] == 1)
        def _(bit=bit):
            first_rows(bit)
    loads[0].wait()

    @pl.when(answers[1] == 1)
    def _():
        first_rows(1)

    drain(tiles.at[0, pl.ds(0, 8)], load_sem.at[1])
    for m in range(16):
        z, y, e = peer(m)
        for l in range(2):
            hit = ids[...] == 2 * (e * 4 + y * 2 + z) + l
            row = jnp.sum(jnp.where(hit, gates[...], 0.0), axis=0, keepdims=True)
            for q in range(4):
                tiles[0, m, pl.ds(2 * q + l, 1), :] = row[:, q * QUARTER:(q + 1) * QUARTER]
    for i, bit in enumerate(BITS):
        @pl.when(answers[bit] == 0)
        def _(i=i, bit=bit):
            pl.semaphore_wait(ready.at[i], 1)
            first_rows(bit)
    tiles_start(0)
    tiles_start(1)
    gather_start(1)
    gather_start(2)
    drain(x_all.at[pl.ds(0, 6)], load_sem.at[2])
    tiles_wait(0)

    def merge_tiles(w):
        token = lax.broadcasted_iota(jnp.int32, (8, QUARTER), 0) // 2 * QUARTER + lax.broadcasted_iota(jnp.int32, (8, QUARTER), 1)
        for side in range(2):
            tile = None
            for part in PARTS:
                m = masks(part)[w] | side
                mine = tiles[len(PATHS[m]), m]
                tile = mine if tile is None else jnp.where(token < part[0], tile, mine)
            merged[2 * w + side] = tile

    def before(j):
        for g, onward in {1: ((1, (2, 3)),), 2: ((2, ()),), 7: ((3, (4, 5)),), 8: ((4, ()),), 13: ((5, (6,)),), 14: ((6, ()),)}.get(j, ()):
            tiles_wait(g)
            for k in onward:
                tiles_start(k)
        if j % 2 == 1 and j < 14:
            w = (j + 1) // 2
            gather_wait(w - 1)
            for k in ONWARD[w - 1]:
                gather_start(k)
            pair_copy(w).start()
        if j % 2 == 0 and j < 16:
            merge_tiles(j // 2)
            pair_copy(j // 2).wait_recv()

    def after(j):
        if j == 7:
            reduce_start(0)
        if j == 10:
            reduce_start(1, PARTS[:3])

    def up(slot, rows):
        for l in range(2):
            for n in range(2):
                cs = slice(n * 256, n * 256 + 256)
                x_in = x_all[slot, rows, :]
                h1 = jnp.dot(x_in, w1[l, :, cs], preferred_element_type=jnp.float32)
                h3 = jnp.dot(x_in, w3[l, :, cs], preferred_element_type=jnp.float32)
                act[l, :, cs] = (h1 * jax.nn.sigmoid(h1) * h3).astype(jnp.bfloat16)

    def down(slot, h, store):
        columns = merged[slot].T
        gate = []
        for l in range(2):
            halves = [jnp.where(h == 0, columns[:, 2 * i + l:2 * i + l + 1], columns[:, 4 + 2 * i + l:5 + 2 * i + l]) for i in range(2)]
            gate.append(jnp.concatenate(halves, axis=0))
        for n in range(4):
            cs = slice(n * 256, n * 256 + 256)
            total = None
            for l in range(2):
                o = jnp.dot(act[l], w2[l, :, cs], preferred_element_type=jnp.float32)
                o = o.astype(jnp.bfloat16).astype(jnp.float32)
                term = jnp.where(gate[l] > 0, gate[l] * o, 0.0)
                total = term if total is None else total + term
            store(cs, total)

    @pl.loop(0, 17)
    def _(i):
        for j in range(16):
            @pl.when(i == j)
            def _(j=j):
                before(j)

        @pl.when(i < 16)
        def _():
            w, h = i // 2, i % 2
            rows = pl.ds(pl.multiple_of(h * HALF, HALF), HALF)

            @pl.when(i >= 2)
            def _():
                partial_copy(h).wait_send()

            up(2 * w + 1, rows)

            def store(cs, total):
                dd_out[h, :, cs] = total

            down(2 * w + 1, h, store)

            @pl.when(i >= 2)
            def _():
                pl.semaphore_wait(ready.at[3 * h], 1)

            partial_copy(h).start()

        @pl.when(i > 0)
        def _():
            w, h = (i - 1) // 2, (i - 1) % 2
            rows = pl.ds(pl.multiple_of(h * HALF, HALF), HALF)
            up(2 * w, rows)
            partial_copy(h).wait_recv()

            def store(cs, total):
                acc[w, rows, cs] = total + dd_in[h, :, cs]

            down(2 * w, h, store)

            @pl.when(i < 15)
            def _():
                pl.semaphore_signal(ready.at[3 * h], inc=1, device_id=peer(1), device_id_type=MESH)

        for j in (7, 10):
            @pl.when(i == j)
            def _(j=j):
                after(j)

    reduce_start(1, PARTS[3:])
    reduce_start(2)
    reduce_start(3)

    def sum_rows(first, n, fn):
        @pl.loop(0, n // 16)
        def _(i):
            fn(pl.ds(pl.multiple_of(first + i * 16, 16), 16))

    def add(k):
        reduce_wait(k)
        for first, n, part in ((0, 480, PARTS[0]), (480, 16, PARTS[3]), (496, 16, PARTS[4])):
            w = reduce_move(part, k)[1]

            def one(rows, w=w):
                got = acc[w, rows, :] + rs[k, rows, :]
                if k == 5:
                    got = got + x_all[0, rows, :].astype(jnp.float32)
                acc[w, rows, :] = got

            sum_rows(first, n, one)

    add(0)
    add(1)
    add(2)
    reduce_start(4)
    reduce_start(5)
    add(3)
    add(4)
    core = lax.axis_index('ex') % 2

    @pl.when(core == 0)
    def _():
        reduce_last_start()

    add(5)

    @pl.when(core == 1)
    def _():
        reduce_last_start()


    drain(tiles.at[pl.ds(0, 2)], gt_send)
    drain(x_all.at[pl.ds(0, 15)], ag_send)
    for h in range(2):
        partial_copy(h).wait_send()

    def one(rows):
        y_out[rows, :] = (acc[0, rows, :] + rs[6, rows, :]).astype(y_out.dtype)

    reduce_wait(6)
    for r, n, _ in FIRST:
        sum_rows(r, n, one)
    drain(acc.at[pl.ds(0, 7)], rs_send)
    reduce_wait(7)
    for r, n, _ in SECOND:
        one(pl.ds(r, n))


def solution(mesh):
    n_dev = mesh.shape['ez'] * mesh.shape['ey'] * mesh.shape['ex']

    def local_layer(x_loc, ids_loc, gates_loc, w_g, w_u, w_d):
        tok, hid = x_loc.shape
        top_k = ids_loc.shape[1]
        n_local, _, ffn = w_g.shape
        hbm = pl.BlockSpec(memory_space=pl.ANY)
        dma = pltpu.SemaphoreType.DMA
        f32, bf16 = jnp.float32, jnp.bfloat16
        y = pl.pallas_call(
            moe_kernel,
            out_shape=pltpu.VMEM((tok, hid), bf16),
            in_specs=[hbm] * 6,
            out_specs=pl.BlockSpec(memory_space=pltpu.VMEM),
            scratch_shapes=[
                pltpu.VMEM((n_local, hid, ffn), bf16),
                pltpu.VMEM((n_local, hid, ffn), bf16),
                pltpu.VMEM((n_local, ffn, hid), bf16),
                pltpu.VMEM((top_k, tok), jnp.int32),
                pltpu.VMEM((top_k, tok), f32),
                pltpu.VMEM((n_dev, tok, hid), bf16),
                pltpu.VMEM((5, n_dev, 8, QUARTER), f32),
                pltpu.VMEM((n_dev, 8, QUARTER), f32),
                pltpu.VMEM((n_local, HALF, ffn), bf16),
                pltpu.VMEM((8, tok, hid), f32),
                pltpu.VMEM((7, tok, hid), f32),
                pltpu.VMEM((2, HALF, hid), f32),
                pltpu.VMEM((2, HALF, hid), f32),
                dma((4,)), dma, dma((6,)), dma, dma((7,)), dma((2,)),
                dma, pltpu.SemaphoreType.REGULAR((4,)),
            ],
            compiler_params=pltpu.CompilerParams(collective_id=0, has_side_effects=True, vmem_limit_bytes=62_000_000),
            name='moe_kernel',
        )(x_loc, ids_loc.T, gates_loc.T, w_g, w_u, w_d)
        return y

    tok_spec = P(TOKEN_AXES, None)
    w_spec = P(EXPERT_AXES, None, None)
    return jax.shard_map(local_layer, mesh=mesh, in_specs=(tok_spec, tok_spec, tok_spec, w_spec, w_spec, w_spec), out_specs=tok_spec, check_vma=False)
```

```python
import jax
import jax.numpy as jnp
from jax import lax
from jax.experimental import pallas as pl
from jax.experimental.pallas import tpu as pltpu
from jax.sharding import PartitionSpec as P

TOKEN_AXES = ('ez', 'ey', 'ex')
EXPERT_AXES = ('ex', 'ey', 'ez')
MESH = pl.DeviceIdType.MESH

PARTS = (
    (0, 160, (2, 4, 8), (2, 4, 8)),
    (160, 160, (4, 8, 2), (4, 8, 2)),
    (320, 160, (8, 2, 4), (8, 2, 4)),
    (480, 16, (2, 4, 8), (2, 8, 4)),
    (496, 16, (2, 4, 8), (4, 2, 8)),
)
GATHER = ((0, 0), (0, 1), (0, 2), (1, 1), (1, 2), (2, 2), (4, 2))
ONWARD = {0: (3, 4), 1: (5,), 2: (), 3: (6,), 4: (), 5: (), 6: ()}


def masks(part):
    a, b, c = part[2]
    return 0, a, b, c, a ^ b, a ^ c, b ^ c, 14


def reduce_move(part, k):
    a, b, c = part[3]
    mask, axis = ((a, a), (a ^ b, a), (14, a), (a ^ c, a), (b ^ c, b), (b, b), (c, c))[k]
    return masks(part).index(mask), masks(part).index(mask ^ axis), axis


FIRST = [(part[0], 144, part) for part in PARTS[:3]] + [(part[0], part[1], part) for part in PARTS[3:]]
SECOND = [(part[0] + 144, 16, part) for part in PARTS[:3]]
SECOND_ROWS = 48
BITS = (2, 4, 8, 1)
PATHS = {m: [b for b in BITS if m & b] for m in range(16)}
TILE_MOVES = (
    [(0, 1)],
    [(0, m) for m in range(2, 16)],
    [(1, m) for m in (3, 5, 9)],
    [(1, m) for m in (6, 7, 10, 11, 12, 13, 14, 15)],
    [(2, m) for m in (7, 11, 13)],
    [(2, m) for m in (14, 15)],
    [(3, 15)],
)
HALF = 256
QUARTER = 128


def peer(mask):
    z, y, e = lax.axis_index('ez'), lax.axis_index('ey'), lax.axis_index('ex')
    x, c = e // 2, e % 2
    z = 1 - z if mask & 8 else z
    y = 1 - y if mask & 4 else y
    x = 1 - x if mask & 2 else x
    c = 1 - c if mask & 1 else c
    return z, y, 2 * x + c


def moe_kernel(x_hbm, ids_hbm, gates_hbm, w1_hbm, w3_hbm, w2_hbm, y_out,
               w1, w3, w2, ids, gates, x_all, tiles, merged, act, acc, rs, dd_out, dd_in,
               load_sem, gt_send, gt_recv, ag_send, ag_recv, xd_recv,
               rs_send, ready):
    tok = x_hbm.shape[0]

    def remote(src, dst, ssem, rsem, mask):
        return pltpu.make_async_remote_copy(src, dst, ssem, rsem, device_id=peer(mask), device_id_type=MESH)

    def drain(ref, sem):
        pltpu.make_async_copy(ref, ref, sem).wait()

    def gather_start(k):
        w, a = GATHER[k]
        for part in PARTS:
            rows = pl.ds(part[0], part[1])
            remote(x_all.at[2 * w, rows], x_all.at[2 * (k + 1), rows], ag_send, ag_recv.at[min(k, 4) if k < 6 else 5], part[2][a]).start()

    def gather_wait(k):
        if k == 4:
            drain(x_all.at[pl.ds(0, 2)], ag_recv.at[4])
        elif k != 5:
            drain(x_all.at[2 * (k + 1)], ag_recv.at[min(k, 5)])

    def pair_copy(w):
        return remote(x_all.at[2 * w], x_all.at[2 * w + 1], ag_send, xd_recv.at[w % 2], 1)

    def sum_sem(k):
        return (gt_recv.at[0], ag_recv.at[0], ag_recv.at[1], ag_recv.at[2], ag_recv.at[3], gt_recv.at[3], gt_recv.at[1], gt_recv.at[2])[k]

    def reduce_start(k, parts=PARTS):
        for part in parts:
            w, _, axis = reduce_move(part, k)
            rows = pl.ds(part[0], part[1])
            remote(acc.at[w, rows], rs.at[k, rows], rs_send, sum_sem(k), axis).start()

    def reduce_last_start():
        for i, piece in enumerate((FIRST, SECOND)):
            for r, n, part in piece:
                w, _, axis = reduce_move(part, 6)
                rows = pl.ds(r, n)
                remote(acc.at[w, rows], rs.at[6, rows], rs_send, sum_sem(6 + i), axis).start()

    def reduce_wait(k):
        rows = tok if k < 6 else SECOND_ROWS if k == 7 else tok - SECOND_ROWS
        drain(acc.at[0, pl.ds(0, rows)], sum_sem(k))

    def partial_copy(s):
        return remote(dd_out.at[s], dd_in.at[s], load_sem.at[2 + s], load_sem.at[s], 1)

    def tiles_start(g):
        for hop, m in TILE_MOVES[g]:
            remote(tiles.at[hop, m], tiles.at[hop + 1, m], gt_send, gt_recv.at[4 if g == 6 else g], PATHS[m][hop]).start()

    def tiles_wait(g):
        drain(tiles.at[0, pl.ds(0, len(TILE_MOVES[g]))], gt_recv.at[4 if g == 6 else g])

    loads = [pltpu.make_async_copy(s, d, load_sem.at[i]) for i, s, d in (
        (0, x_hbm, x_all.at[0]), (1, ids_hbm, ids), (1, gates_hbm, gates), (2, w1_hbm, w1), (2, w3_hbm, w3), (2, w2_hbm, w2))]

    z, y, e = lax.axis_index('ez'), lax.axis_index('ey'), lax.axis_index('ex')
    answers = {8: z, 4: y, 2: e // 2, 1: 1 - e % 2}
    barrier = pltpu.get_barrier_semaphore()
    for bit in BITS:
        @pl.when(answers[bit] == 0)
        def _(bit=bit):
            pl.semaphore_signal(barrier, inc=1, device_id=peer(bit), device_id_type=MESH)
    for c in loads:
        c.start()
    expected = z + y + e // 2 + 1 - e % 2

    @pl.when(expected > 0)
    def _():
        pl.semaphore_wait(barrier, expected)

    for i, bit in enumerate(BITS):
        @pl.when(answers[bit] == 1)
        def _(i=i, bit=bit):
            pl.semaphore_signal(ready.at[i], inc=1, device_id=peer(bit), device_id_type=MESH)

    def first_rows(bit):
        for part in PARTS:
            if part[2][0] == bit:
                rows = pl.ds(part[0], part[1])
                remote(x_hbm.at[rows], x_all.at[2, rows], ag_send, ag_recv.at[0], bit).start()
        if bit == 1:
            pair_copy(0).start()

    for bit in BITS[:3]:
        @pl.when(answers[bit] == 1)
        def _(bit=bit):
            first_rows(bit)
    loads[0].wait()

    @pl.when(answers[1] == 1)
    def _():
        first_rows(1)

    drain(tiles.at[0, pl.ds(0, 8)], load_sem.at[1])
    for m in range(16):
        z, y, e = peer(m)
        for l in range(2):
            hit = ids[...] == 2 * (e * 4 + y * 2 + z) + l
            row = jnp.sum(jnp.where(hit, gates[...], 0.0), axis=0, keepdims=True)
            for q in range(4):
                tiles[0, m, pl.ds(2 * q + l, 1), :] = row[:, q * QUARTER:(q + 1) * QUARTER]
    for i, bit in enumerate(BITS):
        @pl.when(answers[bit] == 0)
        def _(i=i, bit=bit):
            pl.semaphore_wait(ready.at[i], 1)
            first_rows(bit)
    tiles_start(0)
    tiles_start(1)
    gather_start(1)
    gather_start(2)
    drain(x_all.at[pl.ds(0, 6)], load_sem.at[2])
    tiles_wait(0)

    def merge_tiles(w):
        token = lax.broadcasted_iota(jnp.int32, (8, QUARTER), 0) // 2 * QUARTER + lax.broadcasted_iota(jnp.int32, (8, QUARTER), 1)
        for side in range(2):
            tile = None
            for part in PARTS:
                m = masks(part)[w] | side
                mine = tiles[len(PATHS[m]), m]
                tile = mine if tile is None else jnp.where(token < part[0], tile, mine)
            merged[2 * w + side] = tile

    def before(j):
        for g, onward in {1: ((1, (2, 3)),), 2: ((2, ()),), 7: ((3, (4, 5)),), 8: ((4, ()),), 13: ((5, (6,)),), 14: ((6, ()),)}.get(j, ()):
            tiles_wait(g)
            for k in onward:
                tiles_start(k)
        if j % 2 == 1 and j < 14:
            w = (j + 1) // 2
            gather_wait(w - 1)
            for k in ONWARD[w - 1]:
                gather_start(k)
            pair_copy(w).start()
        if j % 2 == 0 and j < 16:
            merge_tiles(j // 2)
            pair_copy(j // 2).wait_recv()

    def after(j):
        if j == 7:
            reduce_start(0)
        if j == 10:
            reduce_start(1, PARTS[:3])

    def up(slot, rows):
        for l in range(2):
            for n in range(2):
                cs = slice(n * 256, n * 256 + 256)
                x_in = x_all[slot, rows, :]
                h1 = jnp.dot(x_in, w1[l, :, cs], preferred_element_type=jnp.float32)
                h3 = jnp.dot(x_in, w3[l, :, cs], preferred_element_type=jnp.float32)
                act[l, :, cs] = (h1 * jax.nn.sigmoid(h1) * h3).astype(jnp.bfloat16)

    def down(slot, h, store):
        columns = merged[slot].T
        gate = []
        for l in range(2):
            halves = [jnp.where(h == 0, columns[:, 2 * i + l:2 * i + l + 1], columns[:, 4 + 2 * i + l:5 + 2 * i + l]) for i in range(2)]
            gate.append(jnp.concatenate(halves, axis=0))
        for n in range(4):
            cs = slice(n * 256, n * 256 + 256)
            total = None
            for l in range(2):
                o = jnp.dot(act[l], w2[l, :, cs], preferred_element_type=jnp.float32)
                o = o.astype(jnp.bfloat16).astype(jnp.float32)
                term = jnp.where(gate[l] > 0, gate[l] * o, 0.0)
                total = term if total is None else total + term
            store(cs, total)

    @pl.loop(0, 17)
    def _(i):
        for j in range(16):
            @pl.when(i == j)
            def _(j=j):
                before(j)

        @pl.when(i < 16)
        def _():
            w, h = i // 2, i % 2
            rows = pl.ds(pl.multiple_of(h * HALF, HALF), HALF)

            @pl.when(i >= 2)
            def _():
                partial_copy(h).wait_send()

            up(2 * w + 1, rows)

            def store(cs, total):
                dd_out[h, :, cs] = total

            down(2 * w + 1, h, store)

            @pl.when(i >= 2)
            def _():
                pl.semaphore_wait(ready.at[3 * h], 1)

            partial_copy(h).start()

        @pl.when(i > 0)
        def _():
            w, h = (i - 1) // 2, (i - 1) % 2
            rows = pl.ds(pl.multiple_of(h * HALF, HALF), HALF)
            up(2 * w, rows)
            partial_copy(h).wait_recv()

            def store(cs, total):
                acc[w, rows, cs] = total + dd_in[h, :, cs]

            down(2 * w, h, store)

            @pl.when(i < 15)
            def _():
                pl.semaphore_signal(ready.at[3 * h], inc=1, device_id=peer(1), device_id_type=MESH)

        for j in (7, 10):
            @pl.when(i == j)
            def _(j=j):
                after(j)

    reduce_start(1, PARTS[3:])
    reduce_start(2)
    reduce_start(3)

    def sum_rows(first, n, fn):
        @pl.loop(0, n // 16)
        def _(i):
            fn(pl.ds(pl.multiple_of(first + i * 16, 16), 16))

    def add(k):
        reduce_wait(k)
        for first, n, part in ((0, 480, PARTS[0]), (480, 16, PARTS[3]), (496, 16, PARTS[4])):
            w = reduce_move(part, k)[1]

            def one(rows, w=w):
                got = acc[w, rows, :] + rs[k, rows, :]
                if k == 5:
                    got = got + x_all[0, rows, :].astype(jnp.float32)
                acc[w, rows, :] = got

            sum_rows(first, n, one)

    add(0)
    add(1)
    add(2)
    reduce_start(4)
    reduce_start(5)
    add(3)
    add(4)
    core = lax.axis_index('ex') % 2

    @pl.when(core == 0)
    def _():
        reduce_last_start()

    add(5)

    @pl.when(core == 1)
    def _():
        reduce_last_start()


    drain(tiles.at[pl.ds(0, 2)], gt_send)
    drain(x_all.at[pl.ds(0, 15)], ag_send)
    for h in range(2):
        partial_copy(h).wait_send()

    def one(rows):
        y_out[rows, :] = (acc[0, rows, :] + rs[6, rows, :]).astype(y_out.dtype)

    reduce_wait(6)
    for r, n, _ in FIRST:
        sum_rows(r, n, one)
    drain(acc.at[pl.ds(0, 7)], rs_send)
    reduce_wait(7)
    for r, n, _ in SECOND:
        one(pl.ds(r, n))


def solution(mesh):
    n_dev = mesh.shape['ez'] * mesh.shape['ey'] * mesh.shape['ex']

    def local_layer(x_loc, ids_loc, gates_loc, w_g, w_u, w_d):
        tok, hid = x_loc.shape
        top_k = ids_loc.shape[1]
        n_local, _, ffn = w_g.shape
        hbm = pl.BlockSpec(memory_space=pl.ANY)
        dma = pltpu.SemaphoreType.DMA
        f32, bf16 = jnp.float32, jnp.bfloat16
        y = pl.pallas_call(
            moe_kernel,
            out_shape=pltpu.VMEM((tok, hid), bf16),
            in_specs=[hbm] * 6,
            out_specs=pl.BlockSpec(memory_space=pltpu.VMEM),
            scratch_shapes=[
                pltpu.VMEM((n_local, hid, ffn), bf16),
                pltpu.VMEM((n_local, hid, ffn), bf16),
                pltpu.VMEM((n_local, ffn, hid), bf16),
                pltpu.VMEM((top_k, tok), jnp.int32),
                pltpu.VMEM((top_k, tok), f32),
                pltpu.VMEM((n_dev, tok, hid), bf16),
                pltpu.VMEM((5, n_dev, 8, QUARTER), f32),
                pltpu.VMEM((n_dev, 8, QUARTER), f32),
                pltpu.VMEM((n_local, HALF, ffn), bf16),
                pltpu.VMEM((8, tok, hid), f32),
                pltpu.VMEM((7, tok, hid), f32),
                pltpu.VMEM((2, HALF, hid), f32),
                pltpu.VMEM((2, HALF, hid), f32),
                dma((4,)), dma, dma((6,)), dma, dma((6,)), dma((2,)),
                dma, pltpu.SemaphoreType.REGULAR((4,)),
            ],
            compiler_params=pltpu.CompilerParams(collective_id=0, has_side_effects=True, vmem_limit_bytes=62_000_000),
            name='moe_kernel',
        )(x_loc, ids_loc.T, gates_loc.T, w_g, w_u, w_d)
        return y

    tok_spec = P(TOKEN_AXES, None)
    w_spec = P(EXPERT_AXES, None, None)
    return jax.shard_map(local_layer, mesh=mesh, in_specs=(tok_spec, tok_spec, tok_spec, w_spec, w_spec, w_spec), out_specs=tok_spec, check_vma=False)
```

```python
import jax
import jax.numpy as jnp
from jax import lax
from jax.experimental import pallas as pl
from jax.experimental.pallas import tpu as pltpu
from jax.sharding import PartitionSpec as P

TOKEN_AXES = ('ez', 'ey', 'ex')
EXPERT_AXES = ('ex', 'ey', 'ez')
MESH = pl.DeviceIdType.MESH

PARTS = (
    (0, 160, (2, 4, 8), (2, 4, 8)),
    (160, 160, (4, 8, 2), (4, 8, 2)),
    (320, 160, (8, 2, 4), (8, 2, 4)),
    (480, 16, (2, 4, 8), (2, 8, 4)),
    (496, 16, (2, 4, 8), (4, 2, 8)),
)
GATHER = ((0, 0), (0, 1), (0, 2), (1, 1), (1, 2), (2, 2), (4, 2))
ONWARD = {0: (3, 4), 1: (5,), 2: (), 3: (6,), 4: (), 5: (), 6: ()}


def masks(part):
    a, b, c = part[2]
    return 0, a, b, c, a ^ b, a ^ c, b ^ c, 14


def reduce_move(part, k):
    a, b, c = part[3]
    mask, axis = ((a, a), (a ^ b, a), (14, a), (a ^ c, a), (b ^ c, b), (b, b), (c, c))[k]
    return masks(part).index(mask), masks(part).index(mask ^ axis), axis


FIRST = [(part[0], 144, part) for part in PARTS[:3]] + [(part[0], part[1], part) for part in PARTS[3:]]
SECOND = [(part[0] + 144, 16, part) for part in PARTS[:3]]
SECOND_ROWS = 48
BITS = (2, 4, 8, 1)
PATHS = {m: [b for b in BITS if m & b] for m in range(16)}
TILE_MOVES = (
    [(0, 1)],
    [(0, m) for m in range(2, 16)],
    [(1, m) for m in (3, 5, 9)],
    [(1, m) for m in (6, 7, 10, 11, 12, 13, 14, 15)],
    [(2, m) for m in (7, 11, 13)],
    [(2, m) for m in (14, 15)],
    [(3, 15)],
)
HALF = 256
QUARTER = 128


def peer(mask):
    z, y, e = lax.axis_index('ez'), lax.axis_index('ey'), lax.axis_index('ex')
    x, c = e // 2, e % 2
    z = 1 - z if mask & 8 else z
    y = 1 - y if mask & 4 else y
    x = 1 - x if mask & 2 else x
    c = 1 - c if mask & 1 else c
    return z, y, 2 * x + c


def moe_kernel(x_hbm, ids_hbm, gates_hbm, w1_hbm, w3_hbm, w2_hbm, y_out,
               w1, w3, w2, ids, gates, x_all, tiles, merged, act, acc, rs, dd_out, dd_in,
               load_sem, gt_send, gt_recv, ag_send, ag_recv, xd_recv,
               rs_send, ready):
    tok = x_hbm.shape[0]

    def remote(src, dst, ssem, rsem, mask):
        return pltpu.make_async_remote_copy(src, dst, ssem, rsem, device_id=peer(mask), device_id_type=MESH)

    def drain(ref, sem):
        pltpu.make_async_copy(ref, ref, sem).wait()

    def gather_start(k):
        w, a = GATHER[k]
        for part in PARTS:
            rows = pl.ds(part[0], part[1])
            remote(x_all.at[2 * w, rows], x_all.at[2 * (k + 1), rows], ag_send, ag_recv.at[min(k, 4) if k < 6 else 5], part[2][a]).start()

    def gather_wait(k):
        if k == 4:
            drain(x_all.at[pl.ds(0, 2)], ag_recv.at[4])
        elif k != 5:
            drain(x_all.at[2 * (k + 1)], ag_recv.at[min(k, 5)])

    def pair_copy(w):
        return remote(x_all.at[2 * w], x_all.at[2 * w + 1], ag_send, xd_recv.at[w % 2], 1)

    def sum_sem(k):
        return (gt_recv.at[0], ag_recv.at[0], ag_recv.at[1], ag_recv.at[2], ag_recv.at[3], gt_recv.at[3], gt_recv.at[1], gt_recv.at[2])[k]

    def reduce_start(k, parts=PARTS):
        for part in parts:
            w, _, axis = reduce_move(part, k)
            rows = pl.ds(part[0], part[1])
            remote(acc.at[w, rows], rs.at[k, rows], rs_send, sum_sem(k), axis).start()

    def reduce_last_start():
        for i, piece in enumerate((FIRST, SECOND)):
            for r, n, part in piece:
                w, _, axis = reduce_move(part, 6)
                rows = pl.ds(r, n)
                remote(acc.at[w, rows], rs.at[6, rows], rs_send, sum_sem(6 + i), axis).start()

    def reduce_wait(k):
        rows = tok if k < 6 else SECOND_ROWS if k == 7 else tok - SECOND_ROWS
        drain(acc.at[0, pl.ds(0, rows)], sum_sem(k))

    def partial_copy(s):
        return remote(dd_out.at[s], dd_in.at[s], load_sem.at[2], load_sem.at[s], 1)

    def tiles_start(g):
        for hop, m in TILE_MOVES[g]:
            remote(tiles.at[hop, m], tiles.at[hop + 1, m], gt_send, gt_recv.at[4 if g == 6 else g], PATHS[m][hop]).start()

    def tiles_wait(g):
        drain(tiles.at[0, pl.ds(0, len(TILE_MOVES[g]))], gt_recv.at[4 if g == 6 else g])

    loads = [pltpu.make_async_copy(s, d, load_sem.at[i]) for i, s, d in (
        (0, x_hbm, x_all.at[0]), (1, ids_hbm, ids), (1, gates_hbm, gates), (2, w1_hbm, w1), (2, w3_hbm, w3), (2, w2_hbm, w2))]

    z, y, e = lax.axis_index('ez'), lax.axis_index('ey'), lax.axis_index('ex')
    answers = {8: z, 4: y, 2: e // 2, 1: 1 - e % 2}
    barrier = pltpu.get_barrier_semaphore()
    for bit in BITS:
        @pl.when(answers[bit] == 0)
        def _(bit=bit):
            pl.semaphore_signal(barrier, inc=1, device_id=peer(bit), device_id_type=MESH)
    for c in loads:
        c.start()
    expected = z + y + e // 2 + 1 - e % 2

    @pl.when(expected > 0)
    def _():
        pl.semaphore_wait(barrier, expected)

    for i, bit in enumerate(BITS):
        @pl.when(answers[bit] == 1)
        def _(i=i, bit=bit):
            pl.semaphore_signal(ready.at[i], inc=1, device_id=peer(bit), device_id_type=MESH)

    def first_rows(bit):
        for part in PARTS:
            if part[2][0] == bit:
                rows = pl.ds(part[0], part[1])
                remote(x_hbm.at[rows], x_all.at[2, rows], ag_send, ag_recv.at[0], bit).start()
        if bit == 1:
            pair_copy(0).start()

    for bit in BITS[:3]:
        @pl.when(answers[bit] == 1)
        def _(bit=bit):
            first_rows(bit)
    loads[0].wait()

    @pl.when(answers[1] == 1)
    def _():
        first_rows(1)

    drain(tiles.at[0, pl.ds(0, 8)], load_sem.at[1])
    for m in range(16):
        z, y, e = peer(m)
        for l in range(2):
            hit = ids[...] == 2 * (e * 4 + y * 2 + z) + l
            row = jnp.sum(jnp.where(hit, gates[...], 0.0), axis=0, keepdims=True)
            for q in range(4):
                tiles[0, m, pl.ds(2 * q + l, 1), :] = row[:, q * QUARTER:(q + 1) * QUARTER]
    for i, bit in enumerate(BITS):
        @pl.when(answers[bit] == 0)
        def _(i=i, bit=bit):
            pl.semaphore_wait(ready.at[i], 1)
            first_rows(bit)
    tiles_start(0)
    tiles_start(1)
    gather_start(1)
    gather_start(2)
    drain(x_all.at[pl.ds(0, 6)], load_sem.at[2])
    tiles_wait(0)

    def merge_tiles(w):
        token = lax.broadcasted_iota(jnp.int32, (8, QUARTER), 0) // 2 * QUARTER + lax.broadcasted_iota(jnp.int32, (8, QUARTER), 1)
        for side in range(2):
            tile = None
            for part in PARTS:
                m = masks(part)[w] | side
                mine = tiles[len(PATHS[m]), m]
                tile = mine if tile is None else jnp.where(token < part[0], tile, mine)
            merged[2 * w + side] = tile

    def before(j):
        for g, onward in {1: ((1, (2, 3)),), 2: ((2, ()),), 7: ((3, (4, 5)),), 8: ((4, ()),), 13: ((5, (6,)),), 14: ((6, ()),)}.get(j, ()):
            tiles_wait(g)
            for k in onward:
                tiles_start(k)
        if j % 2 == 1 and j < 14:
            w = (j + 1) // 2
            gather_wait(w - 1)
            for k in ONWARD[w - 1]:
                gather_start(k)
            pair_copy(w).start()
        if j % 2 == 0 and j < 16:
            merge_tiles(j // 2)
            pair_copy(j // 2).wait_recv()

    def after(j):
        if j == 7:
            reduce_start(0)
        if j == 10:
            reduce_start(1, PARTS[:3])

    def up(slot, rows):
        for l in range(2):
            for n in range(2):
                cs = slice(n * 256, n * 256 + 256)
                x_in = x_all[slot, rows, :]
                h1 = jnp.dot(x_in, w1[l, :, cs], preferred_element_type=jnp.float32)
                h3 = jnp.dot(x_in, w3[l, :, cs], preferred_element_type=jnp.float32)
                act[l, :, cs] = (h1 * jax.nn.sigmoid(h1) * h3).astype(jnp.bfloat16)

    def down(slot, h, store):
        columns = merged[slot].T
        gate = []
        for l in range(2):
            halves = [jnp.where(h == 0, columns[:, 2 * i + l:2 * i + l + 1], columns[:, 4 + 2 * i + l:5 + 2 * i + l]) for i in range(2)]
            gate.append(jnp.concatenate(halves, axis=0))
        for n in range(4):
            cs = slice(n * 256, n * 256 + 256)
            total = None
            for l in range(2):
                o = jnp.dot(act[l], w2[l, :, cs], preferred_element_type=jnp.float32)
                o = o.astype(jnp.bfloat16).astype(jnp.float32)
                term = jnp.where(gate[l] > 0, gate[l] * o, 0.0)
                total = term if total is None else total + term
            store(cs, total)

    @pl.loop(0, 17)
    def _(i):
        for j in range(16):
            @pl.when(i == j)
            def _(j=j):
                before(j)

        @pl.when(i < 16)
        def _():
            w, h = i // 2, i % 2
            rows = pl.ds(pl.multiple_of(h * HALF, HALF), HALF)

            @pl.when(i >= 1)
            def _():
                partial_copy(h).wait_send()

            up(2 * w + 1, rows)

            def store(cs, total):
                dd_out[h, :, cs] = total

            down(2 * w + 1, h, store)

            @pl.when(i >= 2)
            def _():
                pl.semaphore_wait(ready.at[3 * h], 1)

            partial_copy(h).start()

        @pl.when(i > 0)
        def _():
            w, h = (i - 1) // 2, (i - 1) % 2
            rows = pl.ds(pl.multiple_of(h * HALF, HALF), HALF)
            up(2 * w, rows)
            partial_copy(h).wait_recv()

            def store(cs, total):
                acc[w, rows, cs] = total + dd_in[h, :, cs]

            down(2 * w, h, store)

            @pl.when(i < 15)
            def _():
                pl.semaphore_signal(ready.at[3 * h], inc=1, device_id=peer(1), device_id_type=MESH)

        for j in (7, 10):
            @pl.when(i == j)
            def _(j=j):
                after(j)

    reduce_start(1, PARTS[3:])
    reduce_start(2)
    reduce_start(3)

    def sum_rows(first, n, fn):
        @pl.loop(0, n // 16)
        def _(i):
            fn(pl.ds(pl.multiple_of(first + i * 16, 16), 16))

    def add(k):
        reduce_wait(k)
        for first, n, part in ((0, 480, PARTS[0]), (480, 16, PARTS[3]), (496, 16, PARTS[4])):
            w = reduce_move(part, k)[1]

            def one(rows, w=w):
                got = acc[w, rows, :] + rs[k, rows, :]
                if k == 5:
                    got = got + x_all[0, rows, :].astype(jnp.float32)
                acc[w, rows, :] = got

            sum_rows(first, n, one)

    add(0)
    add(1)
    add(2)
    reduce_start(4)
    reduce_start(5)
    add(3)
    add(4)
    core = lax.axis_index('ex') % 2

    @pl.when(core == 0)
    def _():
        reduce_last_start()

    add(5)

    @pl.when(core == 1)
    def _():
        reduce_last_start()


    drain(tiles.at[pl.ds(0, 2)], gt_send)
    drain(x_all.at[pl.ds(0, 15)], ag_send)
    partial_copy(0).wait_send()

    def one(rows):
        y_out[rows, :] = (acc[0, rows, :] + rs[6, rows, :]).astype(y_out.dtype)

    reduce_wait(6)
    for r, n, _ in FIRST:
        sum_rows(r, n, one)
    drain(acc.at[pl.ds(0, 7)], rs_send)
    reduce_wait(7)
    for r, n, _ in SECOND:
        one(pl.ds(r, n))


def solution(mesh):
    n_dev = mesh.shape['ez'] * mesh.shape['ey'] * mesh.shape['ex']

    def local_layer(x_loc, ids_loc, gates_loc, w_g, w_u, w_d):
        tok, hid = x_loc.shape
        top_k = ids_loc.shape[1]
        n_local, _, ffn = w_g.shape
        hbm = pl.BlockSpec(memory_space=pl.ANY)
        dma = pltpu.SemaphoreType.DMA
        f32, bf16 = jnp.float32, jnp.bfloat16
        y = pl.pallas_call(
            moe_kernel,
            out_shape=pltpu.VMEM((tok, hid), bf16),
            in_specs=[hbm] * 6,
            out_specs=pl.BlockSpec(memory_space=pltpu.VMEM),
            scratch_shapes=[
                pltpu.VMEM((n_local, hid, ffn), bf16),
                pltpu.VMEM((n_local, hid, ffn), bf16),
                pltpu.VMEM((n_local, ffn, hid), bf16),
                pltpu.VMEM((top_k, tok), jnp.int32),
                pltpu.VMEM((top_k, tok), f32),
                pltpu.VMEM((n_dev, tok, hid), bf16),
                pltpu.VMEM((5, n_dev, 8, QUARTER), f32),
                pltpu.VMEM((n_dev, 8, QUARTER), f32),
                pltpu.VMEM((n_local, HALF, ffn), bf16),
                pltpu.VMEM((8, tok, hid), f32),
                pltpu.VMEM((7, tok, hid), f32),
                pltpu.VMEM((2, HALF, hid), f32),
                pltpu.VMEM((2, HALF, hid), f32),
                dma((3,)), dma, dma((6,)), dma, dma((6,)), dma((2,)),
                dma, pltpu.SemaphoreType.REGULAR((4,)),
            ],
            compiler_params=pltpu.CompilerParams(collective_id=0, has_side_effects=True, vmem_limit_bytes=62_000_000),
            name='moe_kernel',
        )(x_loc, ids_loc.T, gates_loc.T, w_g, w_u, w_d)
        return y

    tok_spec = P(TOKEN_AXES, None)
    w_spec = P(EXPERT_AXES, None, None)
    return jax.shard_map(local_layer, mesh=mesh, in_specs=(tok_spec, tok_spec, tok_spec, w_spec, w_spec, w_spec), out_specs=tok_spec, check_vma=False)
```
